16 devices in a mesh: data: 4 (over z, y), stage: 4 (over x, core).
Axes of the slice: x: 2, y: 2, z: 2, core: 2. Of those that a mesh axis runs over, the one named last changes fastest.
Arguments:
- w_in: float32 [4, 768, 3072], P('stage')
- w_out: float32 [4, 3072, 768], P('stage')
- mom_in: float32 [4, 768, 3072], P('stage')
- mom_out: float32 [4, 3072, 768], P('stage')
- var_in: float32 [4, 768, 3072], P('stage')
- var_out: float32 [4, 3072, 768], P('stage')
- acc_in: float32 [4, 4, 768, 3072], P('data', 'stage')
- acc_out: float32 [4, 4, 3072, 768], P('data', 'stage')
- stage_acts: bfloat16 [4, 8192, 768], P('stage', 'data')
- d_out: bfloat16 [8192, 768], P('data')
- next_x: bfloat16 [16, 8192, 768], P(None, 'data')
- learn_rate: float32 [1], replicated
- max_norm: float32 [1], replicated
Outputs:
- output 1: float32 [4, 768, 3072], P('stage')
- output 2: float32 [4, 3072, 768], P('stage')
- output 3: float32 [4, 768, 3072], P('stage')
- output 4: float32 [4, 3072, 768], P('stage')
- output 5: float32 [4, 768, 3072], P('stage')
- output 6: float32 [4, 3072, 768], P('stage')
- output 7: bfloat16 [16, 8192, 768], P(None, 'data')
All inputs are finite; a program needn't handle non-finite values.
Results may differ from the reference program's by a relative error of at most 0.00652518.
Values are sent between devices in bfloat16 or wider.
A program may use at most 1 GiB of HBM per device.

```python
import jax
import jax.numpy as jnp
from jax import lax

STAGES = 4
REPLICAS = 4
MODEL_DIM = 768
FFN_DIM = 3072
MICRO_TOKENS = 2048
NEXT_MICRO = 16
STEP_COUNT = 10

BETA_ONE = 0.9
BETA_TWO = 0.95
ADAM_EPS = 1e-8
WEIGHT_DECAY = 0.1
NORM_EPS = 1e-6
TOTAL_ROWS = REPLICAS * MICRO_TOKENS


def gelu_tanh(gelu_in):
    return jax.nn.gelu(gelu_in, approximate=True)


def block_forward(row_block, w_first, w_second):
    hidden = jnp.dot(row_block, w_first, preferred_element_type=jnp.float32)
    act_h = gelu_tanh(hidden).astype(jnp.bfloat16)
    branch = jnp.dot(act_h, w_second, preferred_element_type=jnp.float32)
    return (row_block.astype(jnp.float32) + branch).astype(jnp.bfloat16)


def block_backward(grad_val, w_first, w_second, stage_in):
    pre_act = jnp.dot(stage_in, w_first, preferred_element_type=jnp.float32)
    act_h, gelu_vjp = jax.vjp(gelu_tanh, pre_act)
    act_h = act_h.astype(jnp.bfloat16)
    dw_second = jnp.dot(act_h.T, grad_val, preferred_element_type=jnp.float32)
    d_hid = jnp.dot(grad_val, w_second.T, preferred_element_type=jnp.float32)
    d_pre = gelu_vjp(d_hid)[0].astype(jnp.bfloat16)
    dw_first = jnp.dot(stage_in.T, d_pre, preferred_element_type=jnp.float32)
    d_in = grad_val.astype(jnp.float32) + jnp.dot(d_pre, w_first.T, preferred_element_type=jnp.float32)
    return d_in.astype(jnp.bfloat16), dw_first, dw_second


def micro_grads(w_in, w_out, stage_acts, d_out):
    w_first = w_in.astype(jnp.bfloat16)
    w_second = w_out.astype(jnp.bfloat16)
    acts_rep = jnp.transpose(stage_acts.reshape(STAGES, REPLICAS, MICRO_TOKENS, MODEL_DIM), (1, 0, 2, 3))
    grad_rep = d_out.reshape(REPLICAS, MICRO_TOKENS, MODEL_DIM)

    def one_replica(operands):
        acts_one, grad_top = operands

        def layer_step(grad_val, layer_ws):
            d_in, dw_first, dw_second = block_backward(grad_val, layer_ws[0], layer_ws[1], layer_ws[2])
            return d_in, (dw_first, dw_second)

        _, grad_pair = lax.scan(layer_step, grad_top, (w_first, w_second, acts_one), reverse=True)
        return grad_pair

    return lax.map(one_replica, (acts_rep, grad_rep))


def summed_grads(acc_in, acc_out, micro_first, micro_second):
    grad_first = jnp.sum(acc_in + micro_first, axis=0) / REPLICAS
    grad_second = jnp.sum(acc_out + micro_second, axis=0) / REPLICAS
    total_norm = jnp.sqrt(jnp.sum(grad_first * grad_first) + jnp.sum(grad_second * grad_second))
    return grad_first, grad_second, total_norm


def adamw_update(param_old, moment, second, grad_val, clip_coef, lr_value):
    scaled = clip_coef * grad_val
    mom_new = BETA_ONE * moment + (1.0 - BETA_ONE) * scaled
    sec_new = BETA_TWO * second + (1.0 - BETA_TWO) * scaled * scaled
    mom_hat = mom_new / (1.0 - BETA_ONE ** STEP_COUNT)
    sec_hat = sec_new / (1.0 - BETA_TWO ** STEP_COUNT)
    param_new = param_old - lr_value * (mom_hat / (jnp.sqrt(sec_hat) + ADAM_EPS) + WEIGHT_DECAY * param_old)
    return param_new, mom_new, sec_new


def forward_all(w_first, w_second, next_x):
    blocks = next_x.reshape(NEXT_MICRO * REPLICAS, MICRO_TOKENS, MODEL_DIM)

    def one_block(row_block):
        def layer_step(carry_rows, layer_ws):
            return block_forward(carry_rows, layer_ws[0], layer_ws[1]), None

        out_rows, _ = lax.scan(layer_step, row_block, (w_first, w_second))
        return out_rows

    return lax.map(one_block, blocks).reshape(NEXT_MICRO, TOTAL_ROWS, MODEL_DIM)


def setup_inputs(seed: int = 0) -> dict:
    key_list = jax.random.split(jax.random.key(seed), 14)
    w_in = jax.random.normal(key_list[0], (STAGES, MODEL_DIM, FFN_DIM), jnp.float32) * MODEL_DIM ** -0.5
    w_out = jax.random.normal(key_list[1], (STAGES, FFN_DIM, MODEL_DIM), jnp.float32) * (FFN_DIM * STAGES) ** -0.5
    stage_acts = jax.random.normal(key_list[2], (STAGES, TOTAL_ROWS, MODEL_DIM), jnp.float32).astype(jnp.bfloat16)
    d_out = jax.random.normal(key_list[3], (TOTAL_ROWS, MODEL_DIM), jnp.float32).astype(jnp.bfloat16)
    next_x = jax.random.normal(key_list[4], (NEXT_MICRO, TOTAL_ROWS, MODEL_DIM), jnp.float32).astype(jnp.bfloat16)
    micro_first, micro_second = micro_grads(w_in, w_out, stage_acts, d_out)
    rms_first = jnp.sqrt(jnp.mean(micro_first * micro_first, axis=(0, 2, 3)))[None, :, None, None]
    rms_second = jnp.sqrt(jnp.mean(micro_second * micro_second, axis=(0, 2, 3)))[None, :, None, None]
    acc_in = jax.random.normal(key_list[5], micro_first.shape, jnp.float32) * rms_first
    acc_out = jax.random.normal(key_list[6], micro_second.shape, jnp.float32) * rms_second
    grad_first, grad_second, total_norm = summed_grads(acc_in, acc_out, micro_first, micro_second)
    max_norm = total_norm * jax.random.uniform(key_list[7], (1,), jnp.float32, 0.35, 0.65)
    clip_coef = max_norm[0] / (total_norm + NORM_EPS)
    q_first = jnp.sqrt(jnp.mean((clip_coef * grad_first) ** 2, axis=(1, 2)))[:, None, None]
    q_second = jnp.sqrt(jnp.mean((clip_coef * grad_second) ** 2, axis=(1, 2)))[:, None, None]
    mom_in = jax.random.normal(key_list[8], w_in.shape, jnp.float32) * 0.1 * q_first
    mom_out = jax.random.normal(key_list[9], w_out.shape, jnp.float32) * 0.1 * q_second
    var_in = jax.random.uniform(key_list[10], w_in.shape, jnp.float32, 0.5, 1.5) * 0.05 * q_first ** 2
    var_out = jax.random.uniform(key_list[11], w_out.shape, jnp.float32, 0.5, 1.5) * 0.05 * q_second ** 2
    learn_rate = jax.random.uniform(key_list[12], (1,), jnp.float32, 0.6, 1.4) * 0.25 * MODEL_DIM ** -0.5
    return {'w_in': w_in, 'w_out': w_out, 'mom_in': mom_in, 'mom_out': mom_out, 'var_in': var_in, 'var_out': var_out, 'acc_in': acc_in, 'acc_out': acc_out, 'stage_acts': stage_acts, 'd_out': d_out, 'next_x': next_x, 'learn_rate': learn_rate, 'max_norm': max_norm}


def reference(w_in, w_out, mom_in, mom_out, var_in, var_out, acc_in, acc_out, stage_acts, d_out, next_x, learn_rate, max_norm):
    micro_first, micro_second = micro_grads(w_in, w_out, stage_acts, d_out)
    grad_first, grad_second, total_norm = summed_grads(acc_in, acc_out, micro_first, micro_second)
    clip_coef = jnp.minimum(1.0, max_norm[0] / (total_norm + NORM_EPS))
    new_first, mom_first, sec_first = adamw_update(w_in, mom_in, var_in, grad_first, clip_coef, learn_rate[0])
    new_second, mom_second, sec_second = adamw_update(w_out, mom_out, var_out, grad_second, clip_coef, learn_rate[0])
    next_y = forward_all(new_first.astype(jnp.bfloat16), new_second.astype(jnp.bfloat16), next_x)
    return (new_first, new_second, mom_first, mom_second, sec_first, sec_second, next_y)
```

```python
import functools

import jax
import jax.numpy as jnp
from jax import lax
from jax.experimental import pallas as pl
from jax.experimental.pallas import tpu as pltpu
from jax.sharding import PartitionSpec as P

BETA_ONE = 0.9
BETA_TWO = 0.95
ADAM_EPS = 1e-8
WEIGHT_DECAY = 0.1
STEP_COUNT = 10
NORM_EPS = 1e-6
TRANS_DIMS = (((1,), (1,)), ((), ()))
FIRST_DIMS = (((0,), (0,)), ((), ()))
F32 = jnp.float32
BF16 = jnp.bfloat16
TILE = 512
DIM = 768
HALF = 384
FFN = 3072
ROWS = 2048
MIB = 1024 * 1024
ROW_BYTES = 3072
CUBE = 0.044715
ROOT = 0.7978845608
STRIP = 64
VMEM_BIG = 63 * MIB
DMA = pltpu.SemaphoreType.DMA
MESH_ID = pl.DeviceIdType.MESH
ANY = pl.BlockSpec(memory_space=pl.ANY)

STAGES = range(4)
OWN, MATE, FAR, RELAY = STAGES
CORE_PERM = [(s, s ^ MATE) for s in STAGES]
X_PERM = [(s, s ^ FAR) for s in STAGES]
CHUNK_0, CHUNK_1, CHUNK_2 = [(group, 0, ROWS) for group in range(3)]
CHUNK_3, CHUNK_4 = [(3, row, ROWS // 2) for row in (0, ROWS // 2)]
DIAG, SIDE_Y, SIDE_Z, SELF = range(4)
LONG, SHORT, SUMS = range(3)
FIRST, SECOND = range(2)


def gelu_tanh(gelu_in):
    return jax.nn.gelu(gelu_in, approximate=True)


def adamw_update(param_old, moment, second, grad_val, clip_coef, lr_value):
    scaled = clip_coef * grad_val
    mom_new = BETA_ONE * moment + (1.0 - BETA_ONE) * scaled
    sec_new = BETA_TWO * second + (1.0 - BETA_TWO) * scaled * scaled
    mom_hat = mom_new / (1.0 - BETA_ONE ** STEP_COUNT)
    sec_hat = sec_new / (1.0 - BETA_TWO ** STEP_COUNT)
    param_new = param_old - lr_value * (mom_hat / (jnp.sqrt(sec_hat) + ADAM_EPS) + WEIGHT_DECAY * param_old)
    return param_new, mom_new, sec_new


def gelu_kernel(z):
    half = 0.5 * z
    return half + half * jnp.tanh(z * (ROOT + ROOT * CUBE * (z * z)))


def forward_kernel(n_blk, spec, n_side, side_rows, gather, *refs):
    in_next, first_group, row0, n_rows, to_out, has_out_in = spec
    refs = list(refs)
    ends = [sum(k[-1] for k in side_rows[:i]) for i in range(n_side)]
    x_ref = refs.pop(0)
    w_refs = [(refs.pop(0), refs.pop(0)) for _ in range(n_blk)]
    q_ref = refs.pop(0) if gather else None
    side_refs = [refs.pop(0) for _ in range(n_side)]
    if has_out_in:
        refs.pop(0)
    if to_out:
        out_ref = refs.pop(0)
    y_ref = refs.pop(0)
    gathered = [refs.pop(0) for _ in range(2)] if gather else None
    w_buf, x_buf, h_buf, w_sem, x_sem, y_sem, o_sem = refs[:7]
    bounce = refs[7:]
    steps = None
    if gather:
        z_v, m_v = bounce[:2]
        steps = exchange_steps(lambda part: q_ref.at[part], z_v, m_v, bounce[2:9])
    stage = lax.axis_index('stage')
    core = lax.rem(stage, 2)
    n_tiles = n_rows // TILE
    n_mb = max(1, n_rows // ROWS)
    mb_rows = n_rows // n_mb

    def x_copies():
        if not in_next:
            return [pltpu.make_async_copy(x_ref.at[pl.ds(row0, n_rows)], x_buf, x_sem.at[0])]
        return [
            pltpu.make_async_copy(
                x_ref.at[4 * (first_group + q) + stage, pl.ds(row0, mb_rows)],
                x_buf.at[pl.ds(q * mb_rows, mb_rows)], x_sem.at[q])
            for q in range(n_mb)]

    def w_copies(blk):
        own = pl.multiple_of(core * HALF, HALF)
        mate = pl.multiple_of((1 - core) * HALF, HALF)
        return [
            pltpu.make_async_copy(w_refs[blk][0], w_buf.at[blk, :, :, pl.ds(own, HALF)], w_sem.at[blk, 0]),
            pltpu.make_async_copy(w_refs[blk][1], w_buf.at[blk, :, :, pl.ds(mate, HALF)], w_sem.at[blk, 1])]

    for cp in x_copies() + w_copies(0):
        cp.start()
    for cp in x_copies():
        cp.wait()
    if n_side:
        side_buf, si_sem, so_sem = bounce

    def side_in(i):
        return pltpu.make_async_copy(side_refs[i], side_buf.at[pl.ds(ends[i], side_rows[i][-1])], si_sem.at[i])

    def side_out(i):
        flip, group, off, rows = side_rows[i]
        owner = stage if flip == OWN else jnp.bitwise_xor(stage, flip)
        return pltpu.make_async_copy(
            side_buf.at[pl.ds(ends[i], rows)],
            out_ref.at[4 * group + owner, pl.ds(off, rows)], so_sem.at[i])

    def y_copy(t):
        return pltpu.make_async_copy(x_buf.at[pl.ds(pl.multiple_of(t * TILE, TILE), TILE)], y_ref.at[pl.ds(pl.multiple_of(t * TILE, TILE), TILE)], y_sem.at[t])

    def o_copy(t):
        return pltpu.make_async_copy(x_buf.at[pl.ds(pl.multiple_of(t * TILE, TILE), TILE)], out_ref.at[4 * first_group + stage, pl.ds(row0 + pl.multiple_of(t * TILE, TILE), TILE)], o_sem.at[t])

    def blk_body(blk, _):
        for half in range(2):
            pltpu.make_async_copy(w_buf.at[blk, :, :, pl.ds(0, HALF)], w_buf.at[blk, :, :, pl.ds(0, HALF)], w_sem.at[blk, half]).wait()
        for nxt in range(1, n_blk):
            @pl.when(blk == nxt - 1)
            def _():
                for cp in w_copies(nxt):
                    cp.start()

        if n_side:
            @pl.when(blk == 0)
            def _():
                for i in range(n_side):
                    side_in(i).start()

            @pl.when(blk == 2)
            def _():
                for i in range(n_side):
                    side_in(i).wait()
                for i in range(n_side):
                    side_out(i).start()

        def tile_body(t, _):
            rows = pl.ds(pl.multiple_of(t * TILE, TILE), TILE)
            if gather:
                for when, step in ((0, 0), (3, 1), (5, 2), (7, 3)):
                    pl.when(t == when)(steps[step])
            x = x_buf[rows, :]
            for j in range(4):
                z = jnp.dot(x, w_buf[blk, j, 0], preferred_element_type=F32)
                h_buf[:, j * DIM:(j + 1) * DIM] = gelu_kernel(z).astype(BF16)
            acc = jnp.dot(h_buf[...], jnp.concatenate([w_buf[blk, j, 1] for j in range(4)], 0), preferred_element_type=F32)
            x_buf[rows, :] = (x.astype(F32) + acc).astype(BF16)

            @pl.when(jnp.logical_and(blk == n_blk - 1, t > 0))
            def _():
                y_copy(t - 1).start()
                if to_out:
                    o_copy(t - 1).start()
            return 0
        lax.fori_loop(0, n_tiles, tile_body, 0)
        return 0

    lax.fori_loop(0, n_blk, blk_body, 0)
    y_copy(n_tiles - 1).start()
    if to_out:
        o_copy(n_tiles - 1).start()
    if gather:
        keep = [pltpu.make_async_copy(z_v, gathered[0], bounce[9].at[0]), pltpu.make_async_copy(m_v, gathered[1], bounce[9].at[1])]
        keep[0].start()
        steps[4]()
        keep[1].start()
        steps[5]()
        for cp in keep:
            cp.wait()
    for t in range(n_tiles):
        y_copy(t).wait()
        if to_out:
            o_copy(t).wait()
    for i in range(n_side):
        side_out(i).wait()


def run_forward(x, weights, chunk, name, to_out=False, out_buf=None, sides=(), piece=None):
    n_rows = chunk[-1]
    in_next = x.ndim > 2
    has_out_in = out_buf is not None
    side_rows = [(flip,) + where for _, flip, where in sides]
    sides = [rows for rows, _, _ in sides]
    spec = (in_next,) + chunk + (to_out, has_out_in)
    n_blk = len(weights)
    n_tiles = n_rows // TILE
    args = [x] + [w for pair in weights for w in pair] + ([piece] if piece is not None else []) + list(sides) + ([out_buf] if has_out_in else [])
    shapes, alias = [], {}
    if to_out:
        shapes.append(jax.ShapeDtypeStruct((16, ROWS, DIM), BF16))
        if has_out_in:
            alias = {len(args) - 1: 0}
    shapes.append(jax.ShapeDtypeStruct((n_rows, DIM), BF16))
    gather = piece is not None
    if gather:
        shapes += [jax.ShapeDtypeStruct((4, 2, HALF, DIM), BF16)] * 2
    scratch = [
        pltpu.VMEM((n_blk, 4, 2, DIM, DIM), BF16),
        pltpu.VMEM((n_rows, DIM), BF16),
        pltpu.VMEM((TILE, FFN), BF16),
        DMA((n_blk, 2)),
        DMA((2,)),
        ] + [DMA((n_tiles,))] * 2
    if gather:
        scratch += EXCHANGE_BUFS + EXCHANGE_SEMS + [DMA((2,))]
    if sides:
        scratch += [pltpu.VMEM((sum(k[-1] for k in side_rows), DIM), BF16), DMA((len(sides),)), DMA((len(sides),))]
    flops = n_rows * n_blk * 4 * DIM * FFN
    res = pl.pallas_call(
        functools.partial(forward_kernel, n_blk, spec, len(sides), tuple(side_rows), gather),
        out_shape=shapes, in_specs=[ANY] * len(args), out_specs=[ANY] * len(shapes),
        scratch_shapes=scratch, input_output_aliases=alias, name=name,
        cost_estimate=pl.CostEstimate(flops=flops, bytes_accessed=n_blk * 9 * MIB + n_rows * FFN, transcendentals=n_rows * n_blk * FFN),
        compiler_params=pltpu.CompilerParams(vmem_limit_bytes=VMEM_BIG, has_side_effects=gather),
    )(*args)
    return res if len(res) > 1 else res[0]


def copy_kernel(n_side, side_rows, *refs):
    side_refs, out_ref = refs[:n_side], refs[n_side + 1]
    side_buf, si_sem, so_sem = refs[n_side + 2:]
    stage = lax.axis_index('stage')
    starts = [sum(k[-1] for k in side_rows[:i]) for i in range(n_side)]

    def cp_in(i):
        return pltpu.make_async_copy(side_refs[i], side_buf.at[pl.ds(starts[i], side_rows[i][-1])], si_sem.at[i])

    def cp_out(i):
        flip, group, off, rows = side_rows[i]
        owner = stage if flip == OWN else jnp.bitwise_xor(stage, flip)
        return pltpu.make_async_copy(side_buf.at[pl.ds(starts[i], rows)], out_ref.at[4 * group + owner, pl.ds(off, rows)], so_sem.at[i])

    for i in range(n_side):
        cp_in(i).start()
    for i in range(n_side):
        cp_in(i).wait()
        cp_out(i).start()
    for i in range(n_side):
        cp_out(i).wait()


def run_copy(out_buf, sides, name):
    side_rows = [(flip,) + where for _, flip, where in sides]
    sides = [rows for rows, _, _ in sides]
    n_side = len(sides)
    rows = sum(k[-1] for k in side_rows)
    return pl.pallas_call(
        functools.partial(copy_kernel, n_side, tuple(side_rows)),
        out_shape=jax.ShapeDtypeStruct(out_buf.shape, BF16), in_specs=[ANY] * (n_side + 1), out_specs=ANY,
        scratch_shapes=[pltpu.VMEM((rows, DIM), BF16), DMA((n_side,)), DMA((n_side,))],
        input_output_aliases={n_side: 0}, name=name,
        cost_estimate=pl.CostEstimate(flops=rows * DIM * 300, bytes_accessed=rows * FFN, transcendentals=0),
        compiler_params=pltpu.CompilerParams(vmem_limit_bytes=VMEM_BIG),
    )(*sides, out_buf)


def update_kernel(scal_ref, g_ref, w_ref, m_ref, v_ref, wo_ref, mo_ref, vo_ref):
    w_new, m_new, v_new = adamw_update(w_ref[0], m_ref[0], v_ref[0], g_ref[0], scal_ref[0], scal_ref[1])
    wo_ref[0] = w_new
    mo_ref[0] = m_new
    vo_ref[0] = v_new


def run_update(scal, grad, w, m, v, name):
    rows = 192
    _, n_row, n_col = w.shape
    per = n_row // rows
    if n_col == FFN:
        par = pl.BlockSpec((1, rows, DIM), lambda j, i: (0, i, j))
        grid, g_spec = (4, 4), pl.BlockSpec((1, rows, DIM), lambda j, i: (j, i, 0))
    else:
        par = pl.BlockSpec((1, rows, DIM), lambda j, i: (0, 4 * j + i, 0))
        grid, g_spec = (4, 4), pl.BlockSpec((1, rows, DIM), lambda j, i: (j, i, 0))
    return pl.pallas_call(
        update_kernel, grid=grid,
        in_specs=[pl.BlockSpec(memory_space=pltpu.SMEM), g_spec, par, par, par], out_specs=[par] * 3,
        out_shape=[jax.ShapeDtypeStruct(w.shape, F32)] * 3, name=name,
        cost_estimate=pl.CostEstimate(flops=20_000_000_000, bytes_accessed=7 * 9 * MIB, transcendentals=n_row * n_col),
    )(scal, grad, w, m, v)


def ids():
    stage, rep = lax.axis_index('stage'), lax.axis_index('data')
    core = lax.rem(stage, 2)
    mate = stage + 1 - 2 * core
    return stage, core, rep, mate, [jnp.bitwise_xor(rep, k) for k in range(4)]


def push(src, dst, send_sem, recv_sem, data, stage):
    return pltpu.make_async_remote_copy(src_ref=src, dst_ref=dst, send_sem=send_sem, recv_sem=recv_sem, device_id=(data, stage), device_id_type=MESH_ID)


def exchange_steps(own, z_v, m_v, sems, before=None):
    ys, yr, zs, zr, ms, mr, ls = sems
    stage, _, rep, mate, near = ids()
    y_id, z_id, d_id = near[1:]

    def over_y(src, quarter, part, i):
        return push(src, z_v.at[quarter, part], ys.at[i], yr.at[i], y_id, stage)

    def over_z(src, quarter, part, i):
        return push(src, z_v.at[quarter, part], zs.at[i], zr.at[i], z_id, stage)

    def cross(quarter, part, src=None):
        i = quarter * 2 + part
        src = z_v.at[quarter, part] if src is None else src
        return push(src, m_v.at[quarter, part], ms.at[i], mr.at[i], rep, mate)

    def local(part):
        return pltpu.make_async_copy(own(part), z_v.at[rep, part], ls.at[part])

    def start():
        for part in (FIRST, SECOND):
            if before is not None:
                before(part)
            over_y(own(part), rep, part, part).start()
            over_z(own(part), rep, part, part).start()
            local(part).start()
            cross(rep, part, own(part)).start()

    def first():
        over_y(own(FIRST), y_id, FIRST, FIRST).wait_recv()
        over_z(z_v.at[y_id, FIRST], y_id, FIRST, SUMS).start()
        cross(y_id, FIRST).start()
        over_z(own(FIRST), z_id, FIRST, FIRST).wait_recv()
        cross(z_id, FIRST).start()

    def second():
        over_z(own(SECOND), z_id, SECOND, SECOND).wait_recv()
        over_y(z_v.at[z_id, SECOND], z_id, SECOND, SUMS).start()
        cross(z_id, SECOND).start()
        over_y(own(SECOND), y_id, SECOND, SECOND).wait_recv()
        cross(y_id, SECOND).start()

    def third():
        over_z(own(FIRST), d_id, FIRST, SUMS).wait_recv()
        cross(d_id, FIRST).start()
        over_y(own(SECOND), d_id, SECOND, SUMS).wait_recv()
        cross(d_id, SECOND).start()
        for part in (FIRST, SECOND):
            local(part).wait()

    def last():
        for quarter in range(4):
            for part in (FIRST, SECOND):
                cross(quarter, part).wait_recv()

    def drain():
        for i in range(3):
            over_y(own(FIRST), rep, FIRST, i).wait_send()
            over_z(own(FIRST), rep, FIRST, i).wait_send()
        for quarter in range(4):
            for part in (FIRST, SECOND):
                cross(quarter, part).wait_send()

    return start, first, second, third, last, drain


EXCHANGE_SEMS = [DMA((3,))] * 4 + [DMA((8,))] * 2 + [DMA((2,))]
EXCHANGE_BUFS = [pltpu.VMEM((4, 2, HALF, DIM), BF16)] * 2


def reduce_kernel(h_ref, g_ref, a_ref, p_ref, acc2_ref, acc1_ref, r2_ref, r1_ref,
                  g_v, a_v, b_v, part, ry, rz, in_sem, b_sem, acc_sem, ys, yr, zs, zr, o_sem):
    stage, _, rep, _, near = ids()
    y_id, z_id = near[1], near[2]
    top, low = pl.ds(0, HALF), pl.ds(HALF, HALF)
    fixed = [pltpu.make_async_copy(g_ref, g_v, in_sem.at[0]), pltpu.make_async_copy(a_ref.at[0], a_v, in_sem.at[1])]

    def target(i):
        return jnp.bitwise_xor(rep, jnp.where(i == DIAG, SELF, jnp.where(i == SELF, DIAG, i)))

    def cols(i):
        return pl.ds(pl.multiple_of(target(i) * DIM, DIM), DIM)

    def loads(mat, i):
        slot = lax.rem(i, 2)
        if mat == 0:
            block, acc = h_ref.at[:, cols(i)], acc2_ref.at[0, 0, cols(i), :]
        else:
            block, acc = p_ref.at[:, cols(i)], acc1_ref.at[0, 0, :, cols(i)]
        return [pltpu.make_async_copy(block, b_v.at[slot], b_sem.at[mat, i]), pltpu.make_async_copy(acc, part.at[mat, i], acc_sem.at[mat, i])]

    def over_y(mat, i, rows, k):
        return push(part.at[mat, i, rows, :], ry.at[mat, k], ys.at[mat, k], yr.at[mat, k], y_id, stage)

    def over_z(mat, i, rows, k):
        return push(part.at[mat, i, rows, :], rz.at[mat, k], zs.at[mat, k], zr.at[mat, k], z_id, stage)

    for cp in loads(0, 0) + fixed:
        cp.start()
    for mat in range(2):
        fixed[mat].wait()

        def body(i, _):
            @pl.when(i < SELF)
            def _():
                for cp in loads(mat, i + 1):
                    cp.start()
            if mat == 0:
                @pl.when(i == SELF)
                def _():
                    for cp in loads(1, 0):
                        cp.start()
            for cp in loads(mat, i):
                cp.wait()
            block = b_v[lax.rem(i, 2)]
            lhs, rhs = (block, g_v[...]) if mat == 0 else (a_v[...], block)
            part[mat, i] = part[mat, i] + lax.dot_general(lhs, rhs, FIRST_DIMS, preferred_element_type=F32)

            @pl.when(i == DIAG)
            def _():
                over_y(mat, i, top, LONG).start()
                over_z(mat, i, low, LONG).start()

            @pl.when(i == SIDE_Y)
            def _():
                over_y(mat, i, top, SHORT).start()

            @pl.when(i == SIDE_Z)
            def _():
                over_z(mat, i, low, SHORT).start()
            return 0
        lax.fori_loop(0, 4, body, 0)

    def add(mat, i, base, buf, k):
        def body(t, _):
            rows = pl.ds(pl.multiple_of(t * STRIP, STRIP), STRIP)
            here = pl.ds(pl.multiple_of(base + t * STRIP, STRIP), STRIP)
            part[mat, i, here, :] = part[mat, i, here, :] + buf[mat, k, rows, :]
            return 0
        lax.fori_loop(0, HALF // STRIP, body, 0)

    for mat in range(2):
        over_y(mat, DIAG, top, LONG).wait_recv()
        add(mat, SIDE_Z, 0, ry, LONG)
        over_z(mat, SIDE_Z, top, SUMS).start()
        over_z(mat, DIAG, low, LONG).wait_recv()
        add(mat, SIDE_Y, HALF, rz, LONG)
        over_y(mat, SIDE_Y, low, SUMS).start()
    for mat in range(2):
        over_y(mat, SIDE_Y, top, SHORT).wait_recv()
        add(mat, SELF, 0, ry, SHORT)
        over_z(mat, SIDE_Z, low, SHORT).wait_recv()
        add(mat, SELF, HALF, rz, SHORT)
    outs = [pltpu.make_async_copy(part.at[mat, SELF], ref.at[0], o_sem.at[mat]) for mat, ref in ((0, r2_ref), (1, r1_ref))]
    for mat in range(2):
        over_z(mat, SIDE_Z, top, SUMS).wait_recv()
        add(mat, SELF, 0, rz, SUMS)
        over_y(mat, SIDE_Y, low, SUMS).wait_recv()
        add(mat, SELF, HALF, ry, SUMS)
        outs[mat].start()
    for mat in range(2):
        for k in (LONG, SHORT, SUMS):
            over_y(mat, DIAG, top, k).wait_send()
            over_z(mat, DIAG, top, k).wait_send()
        outs[mat].wait()


def run_reduce(act_h, grad, acts, d_pre, acc_second, acc_first):
    shard = jax.ShapeDtypeStruct((1, DIM, DIM), F32)
    return pl.pallas_call(
        reduce_kernel, in_specs=[ANY] * 6, out_specs=[ANY] * 2, out_shape=[shard, shard], name='reduce',
        scratch_shapes=[pltpu.VMEM((ROWS, DIM), BF16), pltpu.VMEM((ROWS, DIM), BF16), pltpu.VMEM((2, ROWS, DIM), BF16),
                        pltpu.VMEM((2, 4, DIM, DIM), F32), pltpu.VMEM((2, 3, HALF, DIM), F32), pltpu.VMEM((2, 3, HALF, DIM), F32),
                        DMA((2,)), DMA((2, 4)), DMA((2, 4))] + [DMA((2, 3))] * 4 + [DMA((2,))],
        cost_estimate=pl.CostEstimate(flops=150_000_000_000, bytes_accessed=70 * MIB, transcendentals=0),
        compiler_params=pltpu.CompilerParams(vmem_limit_bytes=VMEM_BIG, has_side_effects=True),
    )(act_h, grad, acts, d_pre, acc_second, acc_first)


def gelu_grad(z):
    z_sq = z * z
    t = jnp.tanh(z * (ROOT + ROOT * CUBE * z_sq))
    return 0.5 + 0.5 * t + (0.5 * z) * (1.0 - t * t) * (ROOT + 3.0 * ROOT * CUBE * z_sq)


N_CHUNK = 8


def backward_kernel(a_ref, d_ref, w1_ref, w2_ref, h_ref, dz_ref, g_ref, a_v, w1_v, w2_v, z_v, g_v, h_b, p_b, s_b,
                    in_sem, h_sem, p_sem, o_sem, send_sem, recv_sem):
    stage = lax.axis_index('stage')
    rep = lax.axis_index('data')
    rows = a_v.shape[0] // N_CHUNK
    below = jnp.maximum(stage - 1, 0)
    cp_a = pltpu.make_async_copy(a_ref.at[0], a_v, in_sem.at[0])
    cp_1 = pltpu.make_async_copy(w1_ref, w1_v, in_sem.at[1])
    cp_2 = pltpu.make_async_copy(w2_ref, w2_v, in_sem.at[2])
    cp_a.start()
    cp_1.start()
    cp_2.start()
    n_pre = jnp.where(stage == 3, 0, jnp.where(stage == 2, 4, N_CHUNK))

    def d_copy(k):
        return pltpu.make_async_copy(d_ref.at[pl.ds(pl.multiple_of(k * rows, rows), rows)], g_v.at[k], recv_sem.at[k])

    @pl.when(stage == 3)
    def _():
        def body(k, _):
            d_copy(k).start()
            return 0
        lax.fori_loop(0, N_CHUNK, body, 0)

    def out_copy(buf, ref, sem, k):
        return pltpu.make_async_copy(buf, ref.at[pl.ds(pl.multiple_of(k * rows, rows), rows)], sem.at[k])

    def h_copy(k):
        return out_copy(h_b.at[lax.rem(k, 2)], h_ref, h_sem, k)

    def p_copy(k):
        return out_copy(p_b.at[lax.rem(k, 2)], dz_ref, p_sem, k)

    def g_copy(k):
        return out_copy(g_v.at[k], g_ref, o_sem, k)

    def send(k):
        return push(s_b.at[k], g_v.at[k], send_sem.at[k], recv_sem.at[k], rep, below)

    def z_body(k, _):
        @pl.when(k >= 2)
        def _():
            h_copy(k - 2).wait()
        a = a_v[pl.ds(pl.multiple_of(k * rows, rows), rows), :]
        slot = lax.rem(k, 2)
        for j in range(4):
            cols = slice(j * DIM, (j + 1) * DIM)
            z = jnp.dot(a, w1_v[:, cols], preferred_element_type=F32)
            z_v[k, :, cols] = z
            h_b[slot, :, cols] = gelu_kernel(z).astype(BF16)
        h_copy(k).start()
        return 0

    cp_a.wait()
    cp_1.wait()
    lax.fori_loop(0, n_pre, z_body, 0)
    cp_2.wait()

    def chain_body(k, _):
        lax.fori_loop(k, jnp.where(k >= n_pre, k + 1, k), z_body, 0)
        d_copy(k).wait()

        @pl.when(k >= 2)
        def _():
            p_copy(k - 2).wait()
        g_copy(k).start()
        g = g_v[k]
        slot = lax.rem(k, 2)
        acc = None
        for j in range(4):
            cols = slice(j * DIM, (j + 1) * DIM)
            d_hid = lax.dot_general(g, w2_v[cols, :], TRANS_DIMS, preferred_element_type=F32)
            d_pre = (gelu_grad(z_v[k, :, cols]) * d_hid).astype(BF16)
            p_b[slot, :, cols] = d_pre
            part = lax.dot_general(d_pre, w1_v[:, cols], TRANS_DIMS, preferred_element_type=F32)
            acc = part if acc is None else acc + part
        s_b[k] = (g.astype(F32) + acc).astype(BF16)

        @pl.when(stage > 0)
        def _():
            send(k).start()
        p_copy(k).start()
        return 0

    lax.fori_loop(0, N_CHUNK, chain_body, 0)

    @pl.when(stage > 0)
    def _():
        def body(k, _):
            send(k).wait_send()
            return 0
        lax.fori_loop(0, N_CHUNK, body, 0)
    for k in (N_CHUNK - 2, N_CHUNK - 1):
        h_copy(k).wait()
        p_copy(k).wait()

    def fin(k, _):
        g_copy(k).wait()
        return 0
    lax.fori_loop(0, N_CHUNK, fin, 0)


def run_backward(acts, d_out, w1, w2):
    n = d_out.shape[0]
    rows = n // N_CHUNK
    return pl.pallas_call(
        backward_kernel, in_specs=[ANY] * 4, out_specs=[ANY] * 3, name='backward',
        out_shape=[jax.ShapeDtypeStruct((n, FFN), BF16), jax.ShapeDtypeStruct((n, FFN), BF16), jax.ShapeDtypeStruct((n, DIM), BF16)],
        scratch_shapes=[
            pltpu.VMEM((n, DIM), BF16), pltpu.VMEM((DIM, FFN), BF16), pltpu.VMEM((FFN, DIM), BF16),
            pltpu.VMEM((N_CHUNK, rows, FFN), F32), pltpu.VMEM((N_CHUNK, rows, DIM), BF16),
            pltpu.VMEM((2, rows, FFN), BF16), pltpu.VMEM((2, rows, FFN), BF16), pltpu.VMEM((N_CHUNK, rows, DIM), BF16),
            DMA((3,)), DMA((N_CHUNK,)), DMA((N_CHUNK,)),
            DMA((N_CHUNK,)), DMA((N_CHUNK,)), DMA((N_CHUNK,))],
        cost_estimate=pl.CostEstimate(flops=6 * n * DIM * FFN, bytes_accessed=50_000_000, transcendentals=2 * n * FFN),
        compiler_params=pltpu.CompilerParams(vmem_limit_bytes=VMEM_BIG, has_side_effects=True),
    )(acts, d_out, w1, w2)


def middle_kernel(lr_ref, mx_ref, r1_ref, r2_ref, w1_ref, m1_ref, v1_ref, w2_ref, m2_ref, v2_ref,
                  own_ref, mate_ref, q1_ref, q2_ref, q3_ref, scal_ref,
                  p_v, q_v, z_v, m_v, s_v, n_v, in_sem, ns, nr, hs, hr, xs, xr, o_sem, *sems):
    stage = lax.axis_index('stage')
    rep = lax.axis_index('data')
    core = lax.rem(stage, 2)
    side = lax.div(stage, 2)
    base = 2 * side
    me = rep * 4 + stage

    cols = pl.ds(pl.multiple_of(rep * DIM, DIM), DIM)
    srcs = [r1_ref.at[0], r2_ref.at[0], w1_ref.at[0, :, cols], m1_ref.at[0, :, cols], v1_ref.at[0, :, cols],
            w2_ref.at[0, cols, :], m2_ref.at[0, cols, :], v2_ref.at[0, cols, :]]
    loads = [pltpu.make_async_copy(srcs[i], p_v.at[i], in_sem.at[i]) for i in range(8)]
    for cp in loads:
        cp.start()
    loads[0].wait()
    loads[1].wait()

    def sq_body(t, acc):
        rows = pl.ds(pl.multiple_of(t * 64, 64), 64)
        a = p_v[0, rows, :]
        b = p_v[1, rows, :]
        return acc + a * a + b * b
    acc = lax.fori_loop(0, 12, sq_body, jnp.zeros((64, DIM), F32))
    n_v[me] = jnp.full((8, 128), jnp.sum(acc), F32)

    def norm_send(i, peer):
        return push(n_v.at[me], n_v.at[me], ns.at[i], nr.at[i], lax.div(peer, 4), lax.rem(peer, 4))

    def peer_of(i):
        return lax.rem(me + i, 16)

    for i in range(1, 16):
        norm_send(i, peer_of(i)).start()
    for i in range(1, 16):
        norm_send(i, peer_of(i)).wait()
    total = n_v[0]
    for i in range(1, 16):
        total = total + n_v[i]
    norm = jnp.sqrt(total[0:1, 0:1] * 0.0625)
    clip = jnp.minimum(1.0, mx_ref[0] / (norm + NORM_EPS)) * 0.25
    scal_ref[...] = jnp.broadcast_to(clip, (8, 128))
    for cp in loads[2:]:
        cp.wait()
    lr = lr_ref[0]

    def upd(half, dst):
        for k in range(2):
            def body(t, _):
                rows = pl.ds(pl.multiple_of(half * HALF + t * 64, 64), 64)
                new = adamw_update(p_v[2 + 3 * k, rows, :], p_v[3 + 3 * k, rows, :], p_v[4 + 3 * k, rows, :], p_v[k, rows, :], clip, lr)[0]
                dst[k, pl.ds(pl.multiple_of(t * 64, 64), 64), :] = new.astype(BF16)
                return 0
            lax.fori_loop(0, 6, body, 0)

    mate = base + 1 - core
    far = lax.rem(stage + 2, 4)
    upd(1 - core, s_v)
    half_cp = push(s_v, q_v.at[stage], hs, hr, rep, mate)
    half_cp.start()
    upd(core, q_v.at[stage])
    half_cp.wait_send()
    push(s_v, q_v.at[mate], hs, hr, rep, mate).wait_recv()

    def x_part(blk, i):
        src = q_v.at[blk + i // 2, i % 2]
        return push(src, src, xs.at[i], xr.at[i], rep, far)

    x_out = [x_part(base, i) for i in range(4)]
    x_in = [x_part(2 - base, i) for i in range(4)]
    for cp in x_out:
        cp.start()

    def before(part):
        @pl.when(side == 1)
        def _():
            x_in[part].wait_recv()

    steps = exchange_steps(lambda part: q_v.at[0, part], z_v, m_v, sems, before)
    for step in steps[:4]:
        step()
    outs = [pltpu.make_async_copy(z_v, own_ref, o_sem.at[0])]

    @pl.when(side == 0)
    def _():
        x_in[0].wait_recv()
        x_in[1].wait_recv()
    x_in[2].wait_recv()
    x_in[3].wait_recv()
    outs += [pltpu.make_async_copy(q_v.at[b], r, o_sem.at[b]) for b, r in enumerate((q1_ref, q2_ref, q3_ref), 1)]
    for cp in outs:
        cp.start()
    steps[4]()
    outs.append(pltpu.make_async_copy(m_v, mate_ref, o_sem.at[4]))
    outs[4].start()
    for cp in x_out:
        cp.wait_send()
    steps[5]()
    for cp in outs:
        cp.wait()


def run_middle(lr, mx, r1, r2, w1, m1, v1, w2, m2, v2):
    smem = pl.BlockSpec(memory_space=pltpu.SMEM)
    piece = jax.ShapeDtypeStruct((2, HALF, DIM), BF16)
    block = jax.ShapeDtypeStruct((4, 2, HALF, DIM), BF16)
    return pl.pallas_call(
        middle_kernel, in_specs=[smem, smem] + [ANY] * 8,
        out_specs=[ANY] * 5 + [pl.BlockSpec(memory_space=pltpu.VMEM)],
        out_shape=[block, block, piece, piece, piece, jax.ShapeDtypeStruct((8, 128), F32)], name='middle',
        scratch_shapes=[
            pltpu.VMEM((8, DIM, DIM), F32), pltpu.VMEM((4, 2, HALF, DIM), BF16)] + EXCHANGE_BUFS + [
            pltpu.VMEM((2, HALF, DIM), BF16), pltpu.VMEM((16, 8, 128), F32), DMA((8,)), DMA((16,)), DMA((16,)), DMA, DMA, DMA((4,)), DMA((4,)), DMA((5,))] + EXCHANGE_SEMS,
        cost_estimate=pl.CostEstimate(flops=60_000_000_000, bytes_accessed=40_000_000, transcendentals=0),
        compiler_params=pltpu.CompilerParams(vmem_limit_bytes=VMEM_BIG, has_side_effects=True),
    )(lr, mx, r1, r2, w1, m1, v1, w2, m2, v2)


def solution(mesh):
    w_spec = P('stage', None, None)
    acc_spec = P('data', 'stage', None, None)
    row_spec = P(None, 'data', None)

    def stage_program(w_in, w_out, mom_in, mom_out, var_in, var_out, acc_in, acc_out, stage_acts, d_out, next_x, learn_rate, max_norm):
        w_first = w_in[0].astype(BF16)
        w_second = w_out[0].astype(BF16)
        act_h, pre_keep, grad_keep = run_backward(stage_acts, d_out, w_first, w_second)
        sh_second, sh_first = run_reduce(act_h, grad_keep, stage_acts, pre_keep, acc_out, acc_in)
        own, mate, piece1, piece2, piece3, scal = run_middle(learn_rate, max_norm, sh_first, sh_second, w_in, mom_in, var_in, w_out, mom_out, var_out)
        scal = jnp.stack([scal[0, 0], learn_rate[0]])
        weights = [(own, mate)]
        rows_a = next_x
        both = CHUNK_0[:-1] + (2 * ROWS,)
        for blk, piece in enumerate((piece1, piece2, piece3)):
            rows_a, own, mate = run_forward(rows_a, weights[blk:], both, f'fwd_a{blk}', piece=piece)
            weights.append((own, mate))
        sh_second, sh_first, rows_a = lax.optimization_barrier((sh_second, sh_first, rows_a))
        y_0 = run_forward(rows_a, weights[-1:], CHUNK_0, 'fwd_a3')
        rows_a, y_0 = lax.optimization_barrier((rows_a, y_0))
        y_1 = run_forward(rows_a, weights[-1:], CHUNK_0[:1] + (ROWS, ROWS), 'fwd_a4')

        def to_mate(rows):
            return lax.ppermute(rows, 'stage', CORE_PERM)

        def to_far(rows):
            return lax.ppermute(rows, 'stage', X_PERM)

        far_0, far_1, mate_0, mate_1 = to_far(y_0), to_far(y_1), to_mate(y_0), to_mate(y_1)
        out, y_2 = run_forward(next_x, weights, CHUNK_2, 'fwd_b', to_out=True)
        far_0, mate_0, mate_1, y_2 = lax.optimization_barrier((far_0, mate_0, mate_1, y_2))
        relay_0 = to_mate(far_0)
        far_2, mate_2 = to_far(y_2), to_mate(y_2)
        sides = [(y_0, OWN, CHUNK_0), (y_1, OWN, CHUNK_1), (mate_0, MATE, CHUNK_0), (mate_1, MATE, CHUNK_1)]
        out, y_3 = run_forward(next_x, weights, CHUNK_3, 'fwd_c', to_out=True, out_buf=out, sides=sides)
        far_1, y_3 = lax.optimization_barrier((far_1, y_3))
        relay_1 = to_mate(far_1)
        far_3, mate_3 = to_far(y_3), to_mate(y_3)
        sides = [(far_0, FAR, CHUNK_0), (relay_0, RELAY, CHUNK_0), (mate_2, MATE, CHUNK_2)]
        out, y_4 = run_forward(next_x, weights, CHUNK_4, 'fwd_d', to_out=True, out_buf=out, sides=sides)
        full_second = lax.all_gather(sh_second[0], 'data')
        full_first = lax.all_gather(sh_first[0], 'data')
        scal, y_4 = lax.optimization_barrier((scal, y_4))
        far_4, mate_4 = to_far(y_4), to_mate(y_4)
        new_second, mom_second, sec_second = run_update(scal, full_second, w_out, mom_out, var_out, 'upd_second')
        far_2, new_second, scal = lax.optimization_barrier((far_2, new_second, scal))
        relay_2 = to_mate(far_2)
        new_first, mom_first, sec_first = run_update(scal, full_first, w_in, mom_in, var_in, 'upd_first')
        far_3, new_first = lax.optimization_barrier((far_3, new_first))
        relay_3, relay_4 = to_mate(far_3), to_mate(far_4)
        out = run_copy(out, [(far_1, FAR, CHUNK_1), (relay_1, RELAY, CHUNK_1), (mate_3, MATE, CHUNK_3), (far_2, FAR, CHUNK_2)], 'put_a')
        out = run_copy(out, [(relay_2, RELAY, CHUNK_2), (far_3, FAR, CHUNK_3), (relay_3, RELAY, CHUNK_3), (mate_4, MATE, CHUNK_4), (far_4, FAR, CHUNK_4), (relay_4, RELAY, CHUNK_4)], 'put_b')
        return (new_first, new_second, mom_first, mom_second, sec_first, sec_second, out)

    return jax.shard_map(stage_program, mesh=mesh, in_specs=(w_spec, w_spec, w_spec, w_spec, w_spec, w_spec, acc_spec, acc_spec, P('stage', 'data', None), P('data', None), row_spec, P(None), P(None)), out_specs=(w_spec, w_spec, w_spec, w_spec, w_spec, w_spec, row_spec), check_vma=False)
```

```python
import functools

import jax
import jax.numpy as jnp
from jax import lax
from jax.experimental import pallas as pl
from jax.experimental.pallas import tpu as pltpu
from jax.sharding import PartitionSpec as P

BETA_ONE = 0.9
BETA_TWO = 0.95
ADAM_EPS = 1e-8
WEIGHT_DECAY = 0.1
STEP_COUNT = 10
NORM_EPS = 1e-6
TRANS_DIMS = (((1,), (1,)), ((), ()))
FIRST_DIMS = (((0,), (0,)), ((), ()))
F32 = jnp.float32
BF16 = jnp.bfloat16
TILE = 512
DIM = 768
HALF = 384
FFN = 3072
ROWS = 2048
MIB = 1024 * 1024
ROW_BYTES = 3072
CUBE = 0.044715
ROOT = 0.7978845608
STRIP = 64
VMEM_BIG = 63 * MIB
DMA = pltpu.SemaphoreType.DMA
MESH_ID = pl.DeviceIdType.MESH
ANY = pl.BlockSpec(memory_space=pl.ANY)

STAGES = range(4)
OWN, MATE, FAR, RELAY = STAGES
CORE_PERM = [(s, s ^ MATE) for s in STAGES]
X_PERM = [(s, s ^ FAR) for s in STAGES]
CHUNK_0, CHUNK_1, CHUNK_2 = [(group, 0, ROWS) for group in range(3)]
CHUNK_3, CHUNK_4 = [(3, row, ROWS // 2) for row in (0, ROWS // 2)]
DIAG, SIDE_Y, SIDE_Z, SELF = range(4)
LONG, SHORT, SUMS = range(3)
FIRST, SECOND = range(2)


def gelu_tanh(gelu_in):
    return jax.nn.gelu(gelu_in, approximate=True)


def adamw_update(param_old, moment, second, grad_val, clip_coef, lr_value):
    scaled = clip_coef * grad_val
    mom_new = BETA_ONE * moment + (1.0 - BETA_ONE) * scaled
    sec_new = BETA_TWO * second + (1.0 - BETA_TWO) * scaled * scaled
    mom_hat = mom_new / (1.0 - BETA_ONE ** STEP_COUNT)
    sec_hat = sec_new / (1.0 - BETA_TWO ** STEP_COUNT)
    param_new = param_old - lr_value * (mom_hat / (jnp.sqrt(sec_hat) + ADAM_EPS) + WEIGHT_DECAY * param_old)
    return param_new, mom_new, sec_new


def gelu_kernel(z):
    half = 0.5 * z
    return half + half * jnp.tanh(z * (ROOT + ROOT * CUBE * (z * z)))


def mlp_tile(x_buf, rows, w_v, h_buf):
    x = x_buf[rows, :]
    for j in range(4):
        z = jnp.dot(x, w_v[j, 0], preferred_element_type=F32)
        h_buf[:, j * DIM:(j + 1) * DIM] = gelu_kernel(z).astype(BF16)
    acc = jnp.dot(h_buf[...], jnp.concatenate([w_v[j, 1] for j in range(4)], 0), preferred_element_type=F32)
    x_buf[rows, :] = (x.astype(F32) + acc).astype(BF16)


def forward_kernel(blocks, spec, n_side, side_rows, *refs):
    in_next, first_group, row0, n_rows, to_out, has_out_in = spec
    refs = list(refs)
    ends = [sum(k[-1] for k in side_rows[:i]) for i in range(n_side)]
    x_ref = refs.pop(0)
    w_ref = refs.pop(0)
    n_blk = len(blocks)
    side_refs = [refs.pop(0) for _ in range(n_side)]
    if has_out_in:
        refs.pop(0)
    if to_out:
        out_ref = refs.pop(0)
    y_ref = refs.pop(0)
    w_buf, x_buf, h_buf, w_sem, x_sem, y_sem, o_sem = refs[:7]
    bounce = refs[7:]
    stage = lax.axis_index('stage')
    n_tiles = n_rows // TILE
    n_mb = max(1, n_rows // ROWS)
    mb_rows = n_rows // n_mb

    def x_copies():
        if not in_next:
            return [pltpu.make_async_copy(x_ref.at[pl.ds(row0, n_rows)], x_buf, x_sem.at[0])]
        return [
            pltpu.make_async_copy(
                x_ref.at[4 * (first_group + q) + stage, pl.ds(row0, mb_rows)],
                x_buf.at[pl.ds(q * mb_rows, mb_rows)], x_sem.at[q])
            for q in range(n_mb)]

    def w_copy(blk):
        return pltpu.make_async_copy(w_ref.at[blocks[0] + blk], w_buf.at[blk], w_sem.at[blk])

    for cp in x_copies() + [w_copy(0)]:
        cp.start()
    for cp in x_copies():
        cp.wait()
    if n_side:
        side_buf, si_sem, so_sem = bounce

    def side_in(i):
        return pltpu.make_async_copy(side_refs[i], side_buf.at[pl.ds(ends[i], side_rows[i][-1])], si_sem.at[i])

    def side_out(i):
        flip, group, off, rows = side_rows[i]
        owner = stage if flip == OWN else jnp.bitwise_xor(stage, flip)
        return pltpu.make_async_copy(
            side_buf.at[pl.ds(ends[i], rows)],
            out_ref.at[4 * group + owner, pl.ds(off, rows)], so_sem.at[i])

    def y_copy(t):
        return pltpu.make_async_copy(x_buf.at[pl.ds(pl.multiple_of(t * TILE, TILE), TILE)], y_ref.at[pl.ds(pl.multiple_of(t * TILE, TILE), TILE)], y_sem.at[t])

    def o_copy(t):
        return pltpu.make_async_copy(x_buf.at[pl.ds(pl.multiple_of(t * TILE, TILE), TILE)], out_ref.at[4 * first_group + stage, pl.ds(row0 + pl.multiple_of(t * TILE, TILE), TILE)], o_sem.at[t])

    def blk_body(blk, _):
        w_copy(blk).wait()

        @pl.when(blk < n_blk - 1)
        def _():
            w_copy(blk + 1).start()

        if n_side:
            @pl.when(blk == 0)
            def _():
                for i in range(n_side):
                    side_in(i).start()

            @pl.when(blk == 2)
            def _():
                for i in range(n_side):
                    side_in(i).wait()
                for i in range(n_side):
                    side_out(i).start()

        def tile_body(t, _):
            rows = pl.ds(pl.multiple_of(t * TILE, TILE), TILE)
            mlp_tile(x_buf, rows, w_buf.at[blk], h_buf)

            @pl.when(jnp.logical_and(blk == n_blk - 1, t > 0))
            def _():
                y_copy(t - 1).start()
                if to_out:
                    o_copy(t - 1).start()
            return 0
        lax.fori_loop(0, n_tiles, tile_body, 0)
        return 0

    lax.fori_loop(0, n_blk, blk_body, 0)
    y_copy(n_tiles - 1).start()
    if to_out:
        o_copy(n_tiles - 1).start()
    for t in range(n_tiles):
        y_copy(t).wait()
        if to_out:
            o_copy(t).wait()
    for i in range(n_side):
        side_out(i).wait()


def run_forward(x, weights, chunk, name, to_out=False, out_buf=None, sides=(), blocks=(0, 1, 2, 3)):
    n_rows = chunk[-1]
    in_next = x.ndim > 2
    has_out_in = out_buf is not None
    side_rows = [(flip,) + where for _, flip, where in sides]
    sides = [rows for rows, _, _ in sides]
    spec = (in_next,) + chunk + (to_out, has_out_in)
    n_blk = len(blocks)
    n_tiles = n_rows // TILE
    args = [x, weights] + list(sides) + ([out_buf] if has_out_in else [])
    shapes, alias = [], {}
    if to_out:
        shapes.append(jax.ShapeDtypeStruct((16, ROWS, DIM), BF16))
        if has_out_in:
            alias = {len(args) - 1: 0}
    shapes.append(jax.ShapeDtypeStruct((n_rows, DIM), BF16))
    scratch = [
        pltpu.VMEM((n_blk, 4, 2, DIM, DIM), BF16),
        pltpu.VMEM((n_rows, DIM), BF16),
        pltpu.VMEM((TILE, FFN), BF16),
        DMA((n_blk,)),
        DMA((2,)),
        ] + [DMA((n_tiles,))] * 2
    if sides:
        scratch += [pltpu.VMEM((sum(k[-1] for k in side_rows), DIM), BF16), DMA((len(sides),)), DMA((len(sides),))]
    flops = n_rows * n_blk * 4 * DIM * FFN
    res = pl.pallas_call(
        functools.partial(forward_kernel, tuple(blocks), spec, len(sides), tuple(side_rows)),
        out_shape=shapes, in_specs=[ANY] * len(args), out_specs=[ANY] * len(shapes),
        scratch_shapes=scratch, input_output_aliases=alias, name=name,
        cost_estimate=pl.CostEstimate(flops=flops, bytes_accessed=n_blk * 9 * MIB + n_rows * FFN, transcendentals=n_rows * n_blk * FFN),
        compiler_params=pltpu.CompilerParams(vmem_limit_bytes=VMEM_BIG),
    )(*args)
    return res if len(res) > 1 else res[0]


def copy_kernel(n_side, side_rows, *refs):
    side_refs, out_ref = refs[:n_side], refs[n_side + 1]
    side_buf, si_sem, so_sem = refs[n_side + 2:]
    stage = lax.axis_index('stage')
    starts = [sum(k[-1] for k in side_rows[:i]) for i in range(n_side)]

    def cp_in(i):
        return pltpu.make_async_copy(side_refs[i], side_buf.at[pl.ds(starts[i], side_rows[i][-1])], si_sem.at[i])

    def cp_out(i):
        flip, group, off, rows = side_rows[i]
        owner = stage if flip == OWN else jnp.bitwise_xor(stage, flip)
        return pltpu.make_async_copy(side_buf.at[pl.ds(starts[i], rows)], out_ref.at[4 * group + owner, pl.ds(off, rows)], so_sem.at[i])

    for i in range(n_side):
        cp_in(i).start()
    for i in range(n_side):
        cp_in(i).wait()
        cp_out(i).start()
    for i in range(n_side):
        cp_out(i).wait()


def run_copy(out_buf, sides, name):
    side_rows = [(flip,) + where for _, flip, where in sides]
    sides = [rows for rows, _, _ in sides]
    n_side = len(sides)
    rows = sum(k[-1] for k in side_rows)
    return pl.pallas_call(
        functools.partial(copy_kernel, n_side, tuple(side_rows)),
        out_shape=jax.ShapeDtypeStruct(out_buf.shape, BF16), in_specs=[ANY] * (n_side + 1), out_specs=ANY,
        scratch_shapes=[pltpu.VMEM((rows, DIM), BF16), DMA((n_side,)), DMA((n_side,))],
        input_output_aliases={n_side: 0}, name=name,
        cost_estimate=pl.CostEstimate(flops=rows * DIM * 300, bytes_accessed=rows * FFN, transcendentals=0),
        compiler_params=pltpu.CompilerParams(vmem_limit_bytes=VMEM_BIG),
    )(*sides, out_buf)


def update_kernel(scal_ref, g_ref, w_ref, m_ref, v_ref, wo_ref, mo_ref, vo_ref):
    w_new, m_new, v_new = adamw_update(w_ref[0], m_ref[0], v_ref[0], g_ref[0], scal_ref[0], scal_ref[1])
    wo_ref[0] = w_new
    mo_ref[0] = m_new
    vo_ref[0] = v_new


def run_update(scal, grad, w, m, v, name):
    rows = 192
    _, n_row, n_col = w.shape
    per = n_row // rows
    if n_col == FFN:
        par = pl.BlockSpec((1, rows, DIM), lambda j, i: (0, i, j))
        grid, g_spec = (4, 4), pl.BlockSpec((1, rows, DIM), lambda j, i: (j, i, 0))
    else:
        par = pl.BlockSpec((1, rows, DIM), lambda j, i: (0, 4 * j + i, 0))
        grid, g_spec = (4, 4), pl.BlockSpec((1, rows, DIM), lambda j, i: (j, i, 0))
    return pl.pallas_call(
        update_kernel, grid=grid,
        in_specs=[pl.BlockSpec(memory_space=pltpu.SMEM), g_spec, par, par, par], out_specs=[par] * 3,
        out_shape=[jax.ShapeDtypeStruct(w.shape, F32)] * 3, name=name,
        cost_estimate=pl.CostEstimate(flops=20_000_000_000, bytes_accessed=7 * 9 * MIB, transcendentals=n_row * n_col),
    )(scal, grad, w, m, v)


def ids():
    stage, rep = lax.axis_index('stage'), lax.axis_index('data')
    core = lax.rem(stage, 2)
    mate = stage + 1 - 2 * core
    return stage, core, rep, mate, [jnp.bitwise_xor(rep, k) for k in range(4)]


def push(src, dst, send_sem, recv_sem, data, stage):
    return pltpu.make_async_remote_copy(src_ref=src, dst_ref=dst, send_sem=send_sem, recv_sem=recv_sem, device_id=(data, stage), device_id_type=MESH_ID)


def exchange_steps(own, w_v, sems, before=None):
    ys, yr, zs, zr, ms, mr, ls = sems
    stage, core, rep, mate, near = ids()
    mine = pl.ds(pl.multiple_of(core * HALF, HALF), HALF)

    def z_at(quarter, part):
        return w_v.at[quarter, part, mine, :]

    y_id, z_id, d_id = near[1:]

    def over_y(src, quarter, part, i):
        return push(src, z_at(quarter, part), ys.at[i], yr.at[i], y_id, stage)

    def over_z(src, quarter, part, i):
        return push(src, z_at(quarter, part), zs.at[i], zr.at[i], z_id, stage)

    def cross(quarter, part, src=None):
        i = quarter * 2 + part
        src = z_at(quarter, part) if src is None else src
        return push(src, z_at(quarter, part), ms.at[i], mr.at[i], rep, mate)

    def local(part):
        return pltpu.make_async_copy(own(part), z_at(rep, part), ls.at[part])

    def start():
        for part in (FIRST, SECOND):
            if before is not None:
                before(part)
            over_y(own(part), rep, part, part).start()
            over_z(own(part), rep, part, part).start()
            local(part).start()
            cross(rep, part, own(part)).start()

    def first():
        over_y(own(FIRST), y_id, FIRST, FIRST).wait_recv()
        over_z(z_at(y_id, FIRST), y_id, FIRST, SUMS).start()
        cross(y_id, FIRST).start()
        over_z(own(FIRST), z_id, FIRST, FIRST).wait_recv()
        cross(z_id, FIRST).start()

    def second():
        over_z(own(SECOND), z_id, SECOND, SECOND).wait_recv()
        over_y(z_at(z_id, SECOND), z_id, SECOND, SUMS).start()
        cross(z_id, SECOND).start()
        over_y(own(SECOND), y_id, SECOND, SECOND).wait_recv()
        cross(y_id, SECOND).start()

    def third():
        over_z(own(FIRST), d_id, FIRST, SUMS).wait_recv()
        cross(d_id, FIRST).start()
        over_y(own(SECOND), d_id, SECOND, SUMS).wait_recv()
        cross(d_id, SECOND).start()
        for part in (FIRST, SECOND):
            local(part).wait()

    def last():
        for quarter in range(4):
            for part in (FIRST, SECOND):
                cross(quarter, part).wait_recv()

    def drain():
        for i in range(3):
            over_y(own(FIRST), rep, FIRST, i).wait_send()
            over_z(own(FIRST), rep, FIRST, i).wait_send()
        for quarter in range(4):
            for part in (FIRST, SECOND):
                cross(quarter, part).wait_send()

    return start, first, second, third, last, drain


EXCHANGE_SEMS = [DMA((4, 3))] * 4 + [DMA((4, 8)), DMA((4, 8)), DMA((4, 2))]


def reduce_kernel(h_ref, g_ref, a_ref, p_ref, acc2_ref, acc1_ref, r2_ref, r1_ref,
                  g_v, a_v, b_v, part, ry, rz, in_sem, b_sem, acc_sem, ys, yr, zs, zr, o_sem):
    stage, _, rep, _, near = ids()
    y_id, z_id = near[1], near[2]
    top, low = pl.ds(0, HALF), pl.ds(HALF, HALF)
    fixed = [pltpu.make_async_copy(g_ref, g_v, in_sem.at[0]), pltpu.make_async_copy(a_ref.at[0], a_v, in_sem.at[1])]

    def target(i):
        return jnp.bitwise_xor(rep, jnp.where(i == DIAG, SELF, jnp.where(i == SELF, DIAG, i)))

    def cols(i):
        return pl.ds(pl.multiple_of(target(i) * DIM, DIM), DIM)

    def loads(mat, i):
        slot = lax.rem(i, 2)
        if mat == 0:
            block, acc = h_ref.at[:, cols(i)], acc2_ref.at[0, 0, cols(i), :]
        else:
            block, acc = p_ref.at[:, cols(i)], acc1_ref.at[0, 0, :, cols(i)]
        return [pltpu.make_async_copy(block, b_v.at[slot], b_sem.at[mat, i]), pltpu.make_async_copy(acc, part.at[mat, i], acc_sem.at[mat, i])]

    def over_y(mat, i, rows, k):
        return push(part.at[mat, i, rows, :], ry.at[mat, k], ys.at[mat, k], yr.at[mat, k], y_id, stage)

    def over_z(mat, i, rows, k):
        return push(part.at[mat, i, rows, :], rz.at[mat, k], zs.at[mat, k], zr.at[mat, k], z_id, stage)

    for cp in loads(0, 0) + fixed:
        cp.start()
    for mat in range(2):
        fixed[mat].wait()

        def body(i, _):
            @pl.when(i < SELF)
            def _():
                for cp in loads(mat, i + 1):
                    cp.start()
            if mat == 0:
                @pl.when(i == SELF)
                def _():
                    for cp in loads(1, 0):
                        cp.start()
            for cp in loads(mat, i):
                cp.wait()
            block = b_v[lax.rem(i, 2)]
            lhs, rhs = (block, g_v[...]) if mat == 0 else (a_v[...], block)
            part[mat, i] = part[mat, i] + lax.dot_general(lhs, rhs, FIRST_DIMS, preferred_element_type=F32)

            @pl.when(i == DIAG)
            def _():
                over_y(mat, i, top, LONG).start()
                over_z(mat, i, low, LONG).start()

            @pl.when(i == SIDE_Y)
            def _():
                over_y(mat, i, top, SHORT).start()

            @pl.when(i == SIDE_Z)
            def _():
                over_z(mat, i, low, SHORT).start()
            return 0
        lax.fori_loop(0, 4, body, 0)

    def add(mat, i, base, buf, k):
        def body(t, _):
            rows = pl.ds(pl.multiple_of(t * STRIP, STRIP), STRIP)
            here = pl.ds(pl.multiple_of(base + t * STRIP, STRIP), STRIP)
            part[mat, i, here, :] = part[mat, i, here, :] + buf[mat, k, rows, :]
            return 0
        lax.fori_loop(0, HALF // STRIP, body, 0)

    for mat in range(2):
        over_y(mat, DIAG, top, LONG).wait_recv()
        add(mat, SIDE_Z, 0, ry, LONG)
        over_z(mat, SIDE_Z, top, SUMS).start()
        over_z(mat, DIAG, low, LONG).wait_recv()
        add(mat, SIDE_Y, HALF, rz, LONG)
        over_y(mat, SIDE_Y, low, SUMS).start()
    for mat in range(2):
        over_y(mat, SIDE_Y, top, SHORT).wait_recv()
        add(mat, SELF, 0, ry, SHORT)
        over_z(mat, SIDE_Z, low, SHORT).wait_recv()
        add(mat, SELF, HALF, rz, SHORT)
    outs = [pltpu.make_async_copy(part.at[mat, SELF], ref.at[0], o_sem.at[mat]) for mat, ref in ((0, r2_ref), (1, r1_ref))]
    for mat in range(2):
        over_z(mat, SIDE_Z, top, SUMS).wait_recv()
        add(mat, SELF, 0, rz, SUMS)
        over_y(mat, SIDE_Y, low, SUMS).wait_recv()
        add(mat, SELF, HALF, ry, SUMS)
        outs[mat].start()
    for mat in range(2):
        for k in (LONG, SHORT, SUMS):
            over_y(mat, DIAG, top, k).wait_send()
            over_z(mat, DIAG, top, k).wait_send()
        outs[mat].wait()


def run_reduce(act_h, grad, acts, d_pre, acc_second, acc_first):
    shard = jax.ShapeDtypeStruct((1, DIM, DIM), F32)
    return pl.pallas_call(
        reduce_kernel, in_specs=[ANY] * 6, out_specs=[ANY] * 2, out_shape=[shard, shard], name='reduce',
        scratch_shapes=[pltpu.VMEM((ROWS, DIM), BF16), pltpu.VMEM((ROWS, DIM), BF16), pltpu.VMEM((2, ROWS, DIM), BF16),
                        pltpu.VMEM((2, 4, DIM, DIM), F32), pltpu.VMEM((2, 3, HALF, DIM), F32), pltpu.VMEM((2, 3, HALF, DIM), F32),
                        DMA((2,)), DMA((2, 4)), DMA((2, 4))] + [DMA((2, 3))] * 4 + [DMA((2,))],
        cost_estimate=pl.CostEstimate(flops=150_000_000_000, bytes_accessed=70 * MIB, transcendentals=0),
        compiler_params=pltpu.CompilerParams(vmem_limit_bytes=VMEM_BIG, has_side_effects=True),
    )(act_h, grad, acts, d_pre, acc_second, acc_first)


def gelu_grad(z):
    z_sq = z * z
    t = jnp.tanh(z * (ROOT + ROOT * CUBE * z_sq))
    return 0.5 + 0.5 * t + (0.5 * z) * (1.0 - t * t) * (ROOT + 3.0 * ROOT * CUBE * z_sq)


N_CHUNK = 8


def backward_kernel(a_ref, d_ref, w1_ref, w2_ref, h_ref, dz_ref, g_ref, a_v, w1_v, w2_v, c_v, z_v, g_v, h_b, p_b, s_b,
                    in_sem, w_sem, h_sem, p_sem, o_sem, send_sem, recv_sem):
    stage = lax.axis_index('stage')
    rep = lax.axis_index('data')
    rows = a_v.shape[0] // N_CHUNK
    below = jnp.maximum(stage - 1, 0)
    cp_a = pltpu.make_async_copy(a_ref.at[0], a_v, in_sem.at[0])
    cp_a.start()

    def w_copy(i):
        span = pl.ds((i % 4) * DIM, DIM)
        src = w1_ref.at[0, :, span] if i < 4 else w2_ref.at[0, span, :]
        return pltpu.make_async_copy(src, c_v.at[i % 3], w_sem.at[i])

    for i in range(3):
        w_copy(i).start()
    n_pre = jnp.where(stage == 3, 0, jnp.where(stage == 2, 4, N_CHUNK))

    def d_copy(k):
        return pltpu.make_async_copy(d_ref.at[pl.ds(pl.multiple_of(k * rows, rows), rows)], g_v.at[k], recv_sem.at[k])

    @pl.when(stage == 3)
    def _():
        def body(k, _):
            d_copy(k).start()
            return 0
        lax.fori_loop(0, N_CHUNK, body, 0)

    def out_copy(buf, ref, sem, k):
        return pltpu.make_async_copy(buf, ref.at[pl.ds(pl.multiple_of(k * rows, rows), rows)], sem.at[k])

    def h_copy(k):
        return out_copy(h_b.at[lax.rem(k, 2)], h_ref, h_sem, k)

    def p_copy(k):
        return out_copy(p_b.at[lax.rem(k, 2)], dz_ref, p_sem, k)

    def g_copy(k):
        return out_copy(g_v.at[k], g_ref, o_sem, k)

    def send(k):
        return push(s_b.at[k], g_v.at[k], send_sem.at[k], recv_sem.at[k], rep, below)

    def z_body(k, _):
        @pl.when(k >= 2)
        def _():
            h_copy(k - 2).wait()
        a = a_v[pl.ds(pl.multiple_of(k * rows, rows), rows), :]
        slot = lax.rem(k, 2)
        for j in range(4):
            cols = slice(j * DIM, (j + 1) * DIM)
            z = jnp.dot(a, w1_v[:, cols], preferred_element_type=F32)
            z_v[k, :, cols] = z
            h_b[slot, :, cols] = gelu_kernel(z).astype(BF16)
        h_copy(k).start()
        return 0

    for i in range(8):
        w_copy(i).wait()
        span = slice((i % 4) * DIM, (i % 4 + 1) * DIM)
        if i < 4:
            w1_v[:, span] = c_v[i % 3].astype(BF16)
        else:
            w2_v[span, :] = c_v[i % 3].astype(BF16)
        if i < 5:
            w_copy(i + 3).start()
    cp_a.wait()
    lax.fori_loop(0, n_pre, z_body, 0)

    def chain_body(k, _):
        lax.fori_loop(k, jnp.where(k >= n_pre, k + 1, k), z_body, 0)
        d_copy(k).wait()

        @pl.when(k >= 2)
        def _():
            p_copy(k - 2).wait()
        g_copy(k).start()
        g = g_v[k]
        slot = lax.rem(k, 2)
        acc = None
        for j in range(4):
            cols = slice(j * DIM, (j + 1) * DIM)
            d_hid = lax.dot_general(g, w2_v[cols, :], TRANS_DIMS, preferred_element_type=F32)
            d_pre = (gelu_grad(z_v[k, :, cols]) * d_hid).astype(BF16)
            p_b[slot, :, cols] = d_pre
            part = lax.dot_general(d_pre, w1_v[:, cols], TRANS_DIMS, preferred_element_type=F32)
            acc = part if acc is None else acc + part
        s_b[k] = (g.astype(F32) + acc).astype(BF16)

        @pl.when(stage > 0)
        def _():
            send(k).start()
        p_copy(k).start()
        return 0

    lax.fori_loop(0, N_CHUNK, chain_body, 0)

    @pl.when(stage > 0)
    def _():
        def body(k, _):
            send(k).wait_send()
            return 0
        lax.fori_loop(0, N_CHUNK, body, 0)
    for k in (N_CHUNK - 2, N_CHUNK - 1):
        h_copy(k).wait()
        p_copy(k).wait()

    def fin(k, _):
        g_copy(k).wait()
        return 0
    lax.fori_loop(0, N_CHUNK, fin, 0)


def run_backward(acts, d_out, w1, w2):
    n = d_out.shape[0]
    rows = n // N_CHUNK
    return pl.pallas_call(
        backward_kernel, in_specs=[ANY] * 4, out_specs=[ANY] * 3, name='backward',
        out_shape=[jax.ShapeDtypeStruct((n, FFN), BF16), jax.ShapeDtypeStruct((n, FFN), BF16), jax.ShapeDtypeStruct((n, DIM), BF16)],
        scratch_shapes=[
            pltpu.VMEM((n, DIM), BF16), pltpu.VMEM((DIM, FFN), BF16), pltpu.VMEM((FFN, DIM), BF16), pltpu.VMEM((3, DIM, DIM), F32),
            pltpu.VMEM((N_CHUNK, rows, FFN), F32), pltpu.VMEM((N_CHUNK, rows, DIM), BF16),
            pltpu.VMEM((2, rows, FFN), BF16), pltpu.VMEM((2, rows, FFN), BF16), pltpu.VMEM((N_CHUNK, rows, DIM), BF16),
            DMA((1,)), DMA((8,)), DMA((N_CHUNK,)), DMA((N_CHUNK,)),
            DMA((N_CHUNK,)), DMA((N_CHUNK,)), DMA((N_CHUNK,))],
        cost_estimate=pl.CostEstimate(flops=6 * n * DIM * FFN, bytes_accessed=50_000_000, transcendentals=2 * n * FFN),
        compiler_params=pltpu.CompilerParams(vmem_limit_bytes=VMEM_BIG, has_side_effects=True),
    )(acts, d_out, w1, w2)


def middle_kernel(lr_ref, mx_ref, r1_ref, r2_ref, w1_ref, m1_ref, v1_ref, w2_ref, m2_ref, v2_ref, x_ref,
                  y_ref, all_ref, scal_ref, r_v, p_v, q_v, s_v, n_v, w_v, x_buf, h_buf,
                  r_sem, p_sem, x_sem, ns, nr, hs, hr, xs, xr, o_sem, y_sem, *sems):
    stage, core, rep, mate, _ = ids()
    side = lax.div(stage, 2)
    base = 2 * side
    far = lax.rem(stage + 2, 4)
    me = rep * 4 + stage
    n_dev = 16
    n_tile = x_buf.shape[0] // TILE

    r_loads = [pltpu.make_async_copy(ref.at[0], r_v.at[k], r_sem.at[k]) for k, ref in enumerate((r1_ref, r2_ref))]

    def loads(turn, k):
        half = (1 - core) if turn == 0 else core
        start = pl.multiple_of(rep * DIM, DIM)
        if k == 0:
            refs, where = (w1_ref, m1_ref, v1_ref), (0, pl.ds(pl.multiple_of(half * HALF, HALF), HALF), pl.ds(start, DIM))
        else:
            refs, where = (w2_ref, m2_ref, v2_ref), (0, pl.ds(pl.multiple_of(start + half * HALF, HALF), HALF))
        return [pltpu.make_async_copy(ref.at[where], p_v.at[k, i], p_sem.at[turn, k, i]) for i, ref in enumerate(refs)]

    x_loads = [pltpu.make_async_copy(x_ref.at[4 * q + stage], x_buf.at[pl.ds(q * ROWS, ROWS)], x_sem.at[q]) for q in range(2)]
    for cp in r_loads + loads(0, 0) + loads(0, 1) + x_loads:
        cp.start()
    for cp in r_loads:
        cp.wait()

    def sq_body(t, acc):
        rows = pl.ds(pl.multiple_of(t * STRIP, STRIP), STRIP)
        a = r_v[0, rows, :]
        b = r_v[1, rows, :]
        return acc + a * a + b * b
    acc = lax.fori_loop(0, DIM // STRIP, sq_body, jnp.zeros((STRIP, DIM), F32))
    n_v[me] = jnp.full(n_v.shape[1:], jnp.sum(acc), F32)

    def norm_send(i):
        peer = lax.rem(me + i, n_dev)
        return push(n_v.at[me], n_v.at[me], ns.at[i], nr.at[i], lax.div(peer, 4), lax.rem(peer, 4))

    for i in range(1, n_dev):
        norm_send(i).start()
    for i in range(1, n_dev):
        norm_send(i).wait()
    total = n_v[0]
    for i in range(1, n_dev):
        total = total + n_v[i]
    norm = jnp.sqrt(total[:1, :1] * 0.0625)
    clip = jnp.minimum(1.0, mx_ref[0] / (norm + NORM_EPS)) * 0.25
    scal_ref[...] = jnp.broadcast_to(clip, scal_ref.shape)
    lr = lr_ref[0]

    def upd(turn, dst):
        half = (1 - core) if turn == 0 else core
        for k in range(2):
            for cp in loads(turn, k):
                cp.wait()

            def body(t, _):
                here = pl.ds(pl.multiple_of(t * STRIP, STRIP), STRIP)
                rows = pl.ds(pl.multiple_of(half * HALF + t * STRIP, STRIP), STRIP)
                new = adamw_update(p_v[k, 0, here, :], p_v[k, 1, here, :], p_v[k, 2, here, :], r_v[k, rows, :], clip, lr)[0]
                dst[k, here, :] = new.astype(BF16)
                return 0
            lax.fori_loop(0, HALF // STRIP, body, 0)
            if turn == 0:
                for cp in loads(1, k):
                    cp.start()

    upd(0, s_v)
    half_cp = push(s_v, q_v.at[stage], hs, hr, rep, mate)
    half_cp.start()
    upd(1, q_v.at[stage])
    half_cp.wait_send()
    push(s_v, q_v.at[mate], hs, hr, rep, mate).wait_recv()

    def x_part(blk, i):
        src = q_v.at[blk + i // 2, i % 2]
        return push(src, src, xs.at[i], xr.at[i], rep, far)

    x_out = [x_part(base, i) for i in range(4)]
    x_in = [x_part(2 - base, i) for i in range(4)]
    for cp in x_out:
        cp.start()

    def before(part):
        @pl.when(side == 1)
        def _():
            x_in[part].wait_recv()

    def steps_of(blk, hook=None):
        slot = lax.rem(blk, 3)
        return exchange_steps(lambda part: q_v.at[blk, part], w_v.at[slot], [sem.at[blk] for sem in sems], hook)

    for step in steps_of(0, before):
        step()

    @pl.when(side == 0)
    def _():
        x_in[0].wait_recv()
        x_in[1].wait_recv()
    x_in[2].wait_recv()
    x_in[3].wait_recv()
    for cp in x_out:
        cp.wait_send()
    for cp in x_loads:
        cp.wait()

    def keep(blk):
        return pltpu.make_async_copy(w_v.at[lax.rem(blk, 3)], all_ref.at[blk], o_sem.at[blk])

    def y_copy(t):
        rows = pl.ds(pl.multiple_of(t * TILE, TILE), TILE)
        return pltpu.make_async_copy(x_buf.at[rows], y_ref.at[rows], y_sem.at[t])

    def blk_body(blk, _):
        keep(blk).start()
        steps = steps_of(blk + 1)

        def tile_body(t, _):
            for when, step in zip((0, 3, 5, 7), steps):
                pl.when(t == when)(step)
            mlp_tile(x_buf, pl.ds(pl.multiple_of(t * TILE, TILE), TILE), w_v.at[blk], h_buf)

            @pl.when(jnp.logical_and(blk == 2, t > 0))
            def _():
                y_copy(t - 1).start()
            return 0
        lax.fori_loop(0, n_tile, tile_body, 0)
        for step in steps[4:]:
            step()
        keep(blk).wait()
        return 0

    lax.fori_loop(0, 3, blk_body, 0)
    y_copy(n_tile - 1).start()
    keep(3).start()
    for t in range(n_tile):
        y_copy(t).wait()
    keep(3).wait()


def run_middle(lr, mx, r1, r2, w1, m1, v1, w2, m2, v2, x):
    smem = pl.BlockSpec(memory_space=pltpu.SMEM)
    n_rows = 2 * ROWS
    return pl.pallas_call(
        middle_kernel, in_specs=[smem, smem] + [ANY] * 9,
        out_specs=[ANY] * 2 + [pl.BlockSpec(memory_space=pltpu.VMEM)],
        out_shape=[jax.ShapeDtypeStruct((n_rows, DIM), BF16), jax.ShapeDtypeStruct((4, 4, 2, DIM, DIM), BF16), jax.ShapeDtypeStruct((8, 128), F32)], name='middle',
        scratch_shapes=[
            pltpu.VMEM((2, DIM, DIM), F32), pltpu.VMEM((2, 3, HALF, DIM), F32), pltpu.VMEM((4, 2, HALF, DIM), BF16),
            pltpu.VMEM((2, HALF, DIM), BF16), pltpu.VMEM((16, 8, 128), F32), pltpu.VMEM((3, 4, 2, DIM, DIM), BF16),
            pltpu.VMEM((n_rows, DIM), BF16), pltpu.VMEM((TILE, FFN), BF16),
            DMA((2,)), DMA((2, 2, 3)), DMA((2,)), DMA((16,)), DMA((16,)), DMA, DMA, DMA((4,)), DMA((4,)), DMA((4,)), DMA((n_rows // TILE,))] + EXCHANGE_SEMS,
        cost_estimate=pl.CostEstimate(flops=200_000_000_000, bytes_accessed=100 * MIB, transcendentals=0),
        compiler_params=pltpu.CompilerParams(vmem_limit_bytes=VMEM_BIG, has_side_effects=True),
    )(lr, mx, r1, r2, w1, m1, v1, w2, m2, v2, x)


def solution(mesh):
    w_spec = P('stage', None, None)
    acc_spec = P('data', 'stage', None, None)
    row_spec = P(None, 'data', None)

    def stage_program(w_in, w_out, mom_in, mom_out, var_in, var_out, acc_in, acc_out, stage_acts, d_out, next_x, learn_rate, max_norm):
        act_h, pre_keep, grad_keep = run_backward(stage_acts, d_out, w_in, w_out)
        sh_second, sh_first = run_reduce(act_h, grad_keep, stage_acts, pre_keep, acc_out, acc_in)
        rows_a, weights, scal = run_middle(learn_rate, max_norm, sh_first, sh_second, w_in, mom_in, var_in, w_out, mom_out, var_out, next_x)
        scal = jnp.stack([scal[0, 0], learn_rate[0]])
        sh_second, sh_first, rows_a = lax.optimization_barrier((sh_second, sh_first, rows_a))
        y_0 = run_forward(rows_a, weights, CHUNK_0, 'fwd_a3', blocks=(3,))
        rows_a, y_0 = lax.optimization_barrier((rows_a, y_0))
        y_1 = run_forward(rows_a, weights, CHUNK_0[:1] + (ROWS, ROWS), 'fwd_a4', blocks=(3,))

        def to_mate(rows):
            return lax.ppermute(rows, 'stage', CORE_PERM)

        def to_far(rows):
            return lax.ppermute(rows, 'stage', X_PERM)

        far_0, far_1, mate_0, mate_1 = to_far(y_0), to_far(y_1), to_mate(y_0), to_mate(y_1)
        out, y_2 = run_forward(next_x, weights, CHUNK_2, 'fwd_b', to_out=True)
        far_0, mate_0, mate_1, y_2 = lax.optimization_barrier((far_0, mate_0, mate_1, y_2))
        relay_0 = to_mate(far_0)
        far_2, mate_2 = to_far(y_2), to_mate(y_2)
        sides = [(y_0, OWN, CHUNK_0), (y_1, OWN, CHUNK_1), (mate_0, MATE, CHUNK_0), (mate_1, MATE, CHUNK_1)]
        out, y_3 = run_forward(next_x, weights, CHUNK_3, 'fwd_c', to_out=True, out_buf=out, sides=sides)
        far_1, y_3 = lax.optimization_barrier((far_1, y_3))
        relay_1 = to_mate(far_1)
        far_3, mate_3 = to_far(y_3), to_mate(y_3)
        sides = [(far_0, FAR, CHUNK_0), (relay_0, RELAY, CHUNK_0), (mate_2, MATE, CHUNK_2)]
        out, y_4 = run_forward(next_x, weights, CHUNK_4, 'fwd_d', to_out=True, out_buf=out, sides=sides)
        full_second = lax.all_gather(sh_second[0], 'data')
        full_first = lax.all_gather(sh_first[0], 'data')
        scal, y_4 = lax.optimization_barrier((scal, y_4))
        far_4, mate_4 = to_far(y_4), to_mate(y_4)
        new_second, mom_second, sec_second = run_update(scal, full_second, w_out, mom_out, var_out, 'upd_second')
        far_2, new_second, scal = lax.optimization_barrier((far_2, new_second, scal))
        relay_2 = to_mate(far_2)
        new_first, mom_first, sec_first = run_update(scal, full_first, w_in, mom_in, var_in, 'upd_first')
        far_3, new_first = lax.optimization_barrier((far_3, new_first))
        relay_3, relay_4 = to_mate(far_3), to_mate(far_4)
        out = run_copy(out, [(far_1, FAR, CHUNK_1), (relay_1, RELAY, CHUNK_1), (mate_3, MATE, CHUNK_3), (far_2, FAR, CHUNK_2)], 'put_a')
        out = run_copy(out, [(relay_2, RELAY, CHUNK_2), (far_3, FAR, CHUNK_3), (relay_3, RELAY, CHUNK_3), (mate_4, MATE, CHUNK_4), (far_4, FAR, CHUNK_4), (relay_4, RELAY, CHUNK_4)], 'put_b')
        return (new_first, new_second, mom_first, mom_second, sec_first, sec_second, out)

    return jax.shard_map(stage_program, mesh=mesh, in_specs=(w_spec, w_spec, w_spec, w_spec, w_spec, w_spec, acc_spec, acc_spec, P('stage', 'data', None), P('data', None), row_spec, P(None), P(None)), out_specs=(w_spec, w_spec, w_spec, w_spec, w_spec, w_spec, row_spec), check_vma=False)
```

```python
import functools

import jax
import jax.numpy as jnp
from jax import lax
from jax.experimental import pallas as pl
from jax.experimental.pallas import tpu as pltpu
from jax.sharding import PartitionSpec as P

BETA_ONE = 0.9
BETA_TWO = 0.95
ADAM_EPS = 1e-8
WEIGHT_DECAY = 0.1
STEP_COUNT = 10
NORM_EPS = 1e-6
TRANS_DIMS = (((1,), (1,)), ((), ()))
FIRST_DIMS = (((0,), (0,)), ((), ()))
F32 = jnp.float32
BF16 = jnp.bfloat16
TILE = 512
DIM = 768
HALF = 384
FFN = 3072
ROWS = 2048
MIB = 1024 * 1024
ROW_BYTES = 3072
CUBE = 0.044715
ROOT = 0.7978845608
STRIP = 64
VMEM_BIG = 63 * MIB
DMA = pltpu.SemaphoreType.DMA
MESH_ID = pl.DeviceIdType.MESH
ANY = pl.BlockSpec(memory_space=pl.ANY)

STAGES = range(4)
OWN, MATE, FAR, RELAY = STAGES
CORE_PERM = [(s, s ^ MATE) for s in STAGES]
X_PERM = [(s, s ^ FAR) for s in STAGES]
CHUNK_0, CHUNK_1, CHUNK_2 = [(group, 0, ROWS) for group in range(3)]
CHUNK_3, CHUNK_4 = [(3, row, ROWS // 2) for row in (0, ROWS // 2)]
DIAG, SIDE_Y, SIDE_Z, SELF = range(4)
LONG, SHORT, SUMS = range(3)
FIRST, SECOND = range(2)


def gelu_tanh(gelu_in):
    return jax.nn.gelu(gelu_in, approximate=True)


def adamw_update(param_old, moment, second, grad_val, clip_coef, lr_value):
    scaled = clip_coef * grad_val
    mom_new = BETA_ONE * moment + (1.0 - BETA_ONE) * scaled
    sec_new = BETA_TWO * second + (1.0 - BETA_TWO) * scaled * scaled
    mom_hat = mom_new * (1.0 / (1.0 - BETA_ONE ** STEP_COUNT))
    sec_hat = sec_new * (1.0 / (1.0 - BETA_TWO ** STEP_COUNT))
    param_new = param_old - lr_value * (mom_hat / (jnp.sqrt(sec_hat) + ADAM_EPS) + WEIGHT_DECAY * param_old)
    return param_new, mom_new, sec_new


def gelu_kernel(z):
    half = 0.5 * z
    return half + half * jnp.tanh(z * (ROOT + ROOT * CUBE * (z * z)))


def mlp_tile(x_buf, rows, w_v, h_buf):
    x = x_buf[rows, :]
    for j in range(4):
        z = jnp.dot(x, w_v[j, 0], preferred_element_type=F32)
        h_buf[:, j * DIM:(j + 1) * DIM] = gelu_kernel(z).astype(BF16)
    acc = jnp.dot(h_buf[...], jnp.concatenate([w_v[j, 1] for j in range(4)], 0), preferred_element_type=F32)
    x_buf[rows, :] = (x.astype(F32) + acc).astype(BF16)


def forward_kernel(blocks, spec, n_side, side_rows, *refs):
    in_next, first_group, row0, n_rows, to_out, has_out_in = spec
    refs = list(refs)
    ends = [sum(k[-1] for k in side_rows[:i]) for i in range(n_side)]
    x_ref = refs.pop(0)
    w_ref = refs.pop(0)
    n_blk = len(blocks)
    side_refs = [refs.pop(0) for _ in range(n_side)]
    if has_out_in:
        refs.pop(0)
    if to_out:
        out_ref = refs.pop(0)
    y_ref = refs.pop(0)
    w_buf, x_buf, h_buf, w_sem, x_sem, y_sem, o_sem = refs[:7]
    bounce = refs[7:]
    stage = lax.axis_index('stage')
    n_tiles = n_rows // TILE
    n_mb = max(1, n_rows // ROWS)
    mb_rows = n_rows // n_mb

    def x_copies():
        if not in_next:
            return [pltpu.make_async_copy(x_ref.at[pl.ds(row0, n_rows)], x_buf, x_sem.at[0])]
        return [
            pltpu.make_async_copy(
                x_ref.at[4 * (first_group + q) + stage, pl.ds(row0, mb_rows)],
                x_buf.at[pl.ds(q * mb_rows, mb_rows)], x_sem.at[q])
            for q in range(n_mb)]

    def w_copy(blk):
        return pltpu.make_async_copy(w_ref.at[blocks[0] + blk], w_buf.at[blk], w_sem.at[blk])

    for cp in x_copies() + [w_copy(0)]:
        cp.start()
    for cp in x_copies():
        cp.wait()
    if n_side:
        side_buf, si_sem, so_sem = bounce

    def side_in(i):
        return pltpu.make_async_copy(side_refs[i], side_buf.at[pl.ds(ends[i], side_rows[i][-1])], si_sem.at[i])

    def side_out(i):
        flip, group, off, rows = side_rows[i]
        owner = stage if flip == OWN else jnp.bitwise_xor(stage, flip)
        return pltpu.make_async_copy(
            side_buf.at[pl.ds(ends[i], rows)],
            out_ref.at[4 * group + owner, pl.ds(off, rows)], so_sem.at[i])

    def y_copy(t):
        return pltpu.make_async_copy(x_buf.at[pl.ds(pl.multiple_of(t * TILE, TILE), TILE)], y_ref.at[pl.ds(pl.multiple_of(t * TILE, TILE), TILE)], y_sem.at[t])

    def o_copy(t):
        return pltpu.make_async_copy(x_buf.at[pl.ds(pl.multiple_of(t * TILE, TILE), TILE)], out_ref.at[4 * first_group + stage, pl.ds(row0 + pl.multiple_of(t * TILE, TILE), TILE)], o_sem.at[t])

    def blk_body(blk, _):
        w_copy(blk).wait()

        @pl.when(blk < n_blk - 1)
        def _():
            w_copy(blk + 1).start()

        if n_side:
            @pl.when(blk == 0)
            def _():
                for i in range(n_side):
                    side_in(i).start()

            @pl.when(blk == 2)
            def _():
                for i in range(n_side):
                    side_in(i).wait()
                for i in range(n_side):
                    side_out(i).start()

        def tile_body(t, _):
            rows = pl.ds(pl.multiple_of(t * TILE, TILE), TILE)
            mlp_tile(x_buf, rows, w_buf.at[blk], h_buf)

            @pl.when(jnp.logical_and(blk == n_blk - 1, t > 0))
            def _():
                y_copy(t - 1).start()
                if to_out:
                    o_copy(t - 1).start()
            return 0
        lax.fori_loop(0, n_tiles, tile_body, 0)
        return 0

    lax.fori_loop(0, n_blk, blk_body, 0)
    y_copy(n_tiles - 1).start()
    if to_out:
        o_copy(n_tiles - 1).start()
    for t in range(n_tiles):
        y_copy(t).wait()
        if to_out:
            o_copy(t).wait()
    for i in range(n_side):
        side_out(i).wait()


def run_forward(x, weights, chunk, name, to_out=False, out_buf=None, sides=(), blocks=(0, 1, 2, 3)):
    n_rows = chunk[-1]
    in_next = x.ndim > 2
    has_out_in = out_buf is not None
    side_rows = [(flip,) + where for _, flip, where in sides]
    sides = [rows for rows, _, _ in sides]
    spec = (in_next,) + chunk + (to_out, has_out_in)
    n_blk = len(blocks)
    n_tiles = n_rows // TILE
    args = [x, weights] + list(sides) + ([out_buf] if has_out_in else [])
    shapes, alias = [], {}
    if to_out:
        shapes.append(jax.ShapeDtypeStruct((16, ROWS, DIM), BF16))
        if has_out_in:
            alias = {len(args) - 1: 0}
    shapes.append(jax.ShapeDtypeStruct((n_rows, DIM), BF16))
    scratch = [
        pltpu.VMEM((n_blk, 4, 2, DIM, DIM), BF16),
        pltpu.VMEM((n_rows, DIM), BF16),
        pltpu.VMEM((TILE, FFN), BF16),
        DMA((n_blk,)),
        DMA((2,)),
        ] + [DMA((n_tiles,))] * 2
    if sides:
        scratch += [pltpu.VMEM((sum(k[-1] for k in side_rows), DIM), BF16), DMA((len(sides),)), DMA((len(sides),))]
    flops = n_rows * n_blk * 4 * DIM * FFN
    res = pl.pallas_call(
        functools.partial(forward_kernel, tuple(blocks), spec, len(sides), tuple(side_rows)),
        out_shape=shapes, in_specs=[ANY] * len(args), out_specs=[ANY] * len(shapes),
        scratch_shapes=scratch, input_output_aliases=alias, name=name,
        cost_estimate=pl.CostEstimate(flops=flops, bytes_accessed=n_blk * 9 * MIB + n_rows * FFN, transcendentals=n_rows * n_blk * FFN),
        compiler_params=pltpu.CompilerParams(vmem_limit_bytes=VMEM_BIG),
    )(*args)
    return res if len(res) > 1 else res[0]


def copy_kernel(n_side, side_rows, *refs):
    side_refs, out_ref = refs[:n_side], refs[n_side + 1]
    side_buf, si_sem, so_sem = refs[n_side + 2:]
    stage = lax.axis_index('stage')
    starts = [sum(k[-1] for k in side_rows[:i]) for i in range(n_side)]

    def cp_in(i):
        return pltpu.make_async_copy(side_refs[i], side_buf.at[pl.ds(starts[i], side_rows[i][-1])], si_sem.at[i])

    def cp_out(i):
        flip, group, off, rows = side_rows[i]
        owner = stage if flip == OWN else jnp.bitwise_xor(stage, flip)
        return pltpu.make_async_copy(side_buf.at[pl.ds(starts[i], rows)], out_ref.at[4 * group + owner, pl.ds(off, rows)], so_sem.at[i])

    for i in range(n_side):
        cp_in(i).start()
    for i in range(n_side):
        cp_in(i).wait()
        cp_out(i).start()
    for i in range(n_side):
        cp_out(i).wait()


def run_copy(out_buf, sides, name):
    side_rows = [(flip,) + where for _, flip, where in sides]
    sides = [rows for rows, _, _ in sides]
    n_side = len(sides)
    rows = sum(k[-1] for k in side_rows)
    return pl.pallas_call(
        functools.partial(copy_kernel, n_side, tuple(side_rows)),
        out_shape=jax.ShapeDtypeStruct(out_buf.shape, BF16), in_specs=[ANY] * (n_side + 1), out_specs=ANY,
        scratch_shapes=[pltpu.VMEM((rows, DIM), BF16), DMA((n_side,)), DMA((n_side,))],
        input_output_aliases={n_side: 0}, name=name,
        cost_estimate=pl.CostEstimate(flops=rows * DIM * 300, bytes_accessed=rows * FFN, transcendentals=0),
        compiler_params=pltpu.CompilerParams(vmem_limit_bytes=VMEM_BIG),
    )(*sides, out_buf)


def update_kernel(scal_ref, g_ref, w_ref, m_ref, v_ref, wo_ref, mo_ref, vo_ref):
    w_new, m_new, v_new = adamw_update(w_ref[0], m_ref[0], v_ref[0], g_ref[0], scal_ref[0], scal_ref[1])
    wo_ref[0] = w_new
    mo_ref[0] = m_new
    vo_ref[0] = v_new


def run_update(scal, grad, w, m, v, name):
    rows = HALF
    _, n_row, n_col = w.shape
    per = n_row // rows
    if n_col == FFN:
        par = pl.BlockSpec((1, rows, DIM), lambda j, i: (0, i, j))
        grid, g_spec = (4, 2), pl.BlockSpec((1, rows, DIM), lambda j, i: (j, i, 0))
    else:
        par = pl.BlockSpec((1, rows, DIM), lambda j, i: (0, 2 * j + i, 0))
        grid, g_spec = (4, 2), pl.BlockSpec((1, rows, DIM), lambda j, i: (j, i, 0))
    return pl.pallas_call(
        update_kernel, grid=grid,
        in_specs=[pl.BlockSpec(memory_space=pltpu.SMEM), g_spec, par, par, par], out_specs=[par] * 3,
        out_shape=[jax.ShapeDtypeStruct(w.shape, F32)] * 3, name=name,
        cost_estimate=pl.CostEstimate(flops=20_000_000_000, bytes_accessed=7 * 9 * MIB, transcendentals=n_row * n_col),
        compiler_params=pltpu.CompilerParams(vmem_limit_bytes=VMEM_BIG),
    )(scal, grad, w, m, v)


def ids():
    stage, rep = lax.axis_index('stage'), lax.axis_index('data')
    core = lax.rem(stage, 2)
    mate = stage + 1 - 2 * core
    return stage, core, rep, mate, [jnp.bitwise_xor(rep, k) for k in range(4)]


def push(src, dst, send_sem, recv_sem, data, stage):
    return pltpu.make_async_remote_copy(src_ref=src, dst_ref=dst, send_sem=send_sem, recv_sem=recv_sem, device_id=(data, stage), device_id_type=MESH_ID)


def exchange_steps(own, w_v, sems, before=None):
    ys, yr, zs, zr, ms, mr, ls = sems
    stage, core, rep, mate, near = ids()
    mine = pl.ds(pl.multiple_of(core * HALF, HALF), HALF)

    def z_at(quarter, part):
        return w_v.at[quarter, part, mine, :]

    y_id, z_id, d_id = near[1:]

    def over_y(src, quarter, part, i):
        return push(src, z_at(quarter, part), ys.at[i], yr.at[i], y_id, stage)

    def over_z(src, quarter, part, i):
        return push(src, z_at(quarter, part), zs.at[i], zr.at[i], z_id, stage)

    def cross(quarter, part, src=None):
        i = quarter * 2 + part
        src = z_at(quarter, part) if src is None else src
        return push(src, z_at(quarter, part), ms.at[i], mr.at[i], rep, mate)

    def local(part):
        return pltpu.make_async_copy(own(part), z_at(rep, part), ls.at[part])

    def start():
        for part in (FIRST, SECOND):
            if before is not None:
                before(part)
            over_y(own(part), rep, part, part).start()
            over_z(own(part), rep, part, part).start()
            local(part).start()
            cross(rep, part, own(part)).start()

    def first():
        over_y(own(FIRST), y_id, FIRST, FIRST).wait_recv()
        over_z(z_at(y_id, FIRST), y_id, FIRST, SUMS).start()
        cross(y_id, FIRST).start()
        over_z(own(FIRST), z_id, FIRST, FIRST).wait_recv()
        cross(z_id, FIRST).start()

    def second():
        over_z(own(SECOND), z_id, SECOND, SECOND).wait_recv()
        over_y(z_at(z_id, SECOND), z_id, SECOND, SUMS).start()
        cross(z_id, SECOND).start()
        over_y(own(SECOND), y_id, SECOND, SECOND).wait_recv()
        cross(y_id, SECOND).start()

    def third():
        over_z(own(FIRST), d_id, FIRST, SUMS).wait_recv()
        cross(d_id, FIRST).start()
        over_y(own(SECOND), d_id, SECOND, SUMS).wait_recv()
        cross(d_id, SECOND).start()
        for part in (FIRST, SECOND):
            local(part).wait()

    def last():
        for quarter in range(4):
            for part in (FIRST, SECOND):
                cross(quarter, part).wait_recv()

    def drain():
        for i in range(3):
            over_y(own(FIRST), rep, FIRST, i).wait_send()
            over_z(own(FIRST), rep, FIRST, i).wait_send()
        for quarter in range(4):
            for part in (FIRST, SECOND):
                cross(quarter, part).wait_send()

    return start, first, second, third, last, drain


EXCHANGE_SEMS = [DMA((4, 3))] * 4 + [DMA((4, 8)), DMA((4, 8)), DMA((4, 2))]


def reduce_kernel(h_ref, g_ref, a_ref, p_ref, acc2_ref, acc1_ref, r2_ref, r1_ref,
                  g_v, a_v, b_v, part, ry, rz, in_sem, b_sem, acc_sem, ys, yr, zs, zr, o_sem):
    stage, _, rep, _, near = ids()
    y_id, z_id = near[1], near[2]
    top, low = pl.ds(0, HALF), pl.ds(HALF, HALF)
    fixed = [pltpu.make_async_copy(g_ref, g_v, in_sem.at[0]), pltpu.make_async_copy(a_ref.at[0], a_v, in_sem.at[1])]

    def target(i):
        return jnp.bitwise_xor(rep, jnp.where(i == DIAG, SELF, jnp.where(i == SELF, DIAG, i)))

    def cols(i):
        return pl.ds(pl.multiple_of(target(i) * DIM, DIM), DIM)

    def loads(mat, i):
        slot = lax.rem(i, 2)
        if mat == 0:
            block, acc = h_ref.at[:, cols(i)], acc2_ref.at[0, 0, cols(i), :]
        else:
            block, acc = p_ref.at[:, cols(i)], acc1_ref.at[0, 0, :, cols(i)]
        return [pltpu.make_async_copy(block, b_v.at[slot], b_sem.at[mat, i]), pltpu.make_async_copy(acc, part.at[mat, i], acc_sem.at[mat, i])]

    def over_y(mat, i, rows, k):
        return push(part.at[mat, i, rows, :], ry.at[mat, k], ys.at[mat, k], yr.at[mat, k], y_id, stage)

    def over_z(mat, i, rows, k):
        return push(part.at[mat, i, rows, :], rz.at[mat, k], zs.at[mat, k], zr.at[mat, k], z_id, stage)

    for cp in loads(0, 0) + fixed:
        cp.start()
    for mat in range(2):
        fixed[mat].wait()

        def body(i, _):
            @pl.when(i < SELF)
            def _():
                for cp in loads(mat, i + 1):
                    cp.start()
            if mat == 0:
                @pl.when(i == SELF)
                def _():
                    for cp in loads(1, 0):
                        cp.start()
            for cp in loads(mat, i):
                cp.wait()
            block = b_v[lax.rem(i, 2)]
            lhs, rhs = (block, g_v[...]) if mat == 0 else (a_v[...], block)
            part[mat, i] = part[mat, i] + lax.dot_general(lhs, rhs, FIRST_DIMS, preferred_element_type=F32)

            @pl.when(i == DIAG)
            def _():
                over_y(mat, i, top, LONG).start()
                over_z(mat, i, low, LONG).start()

            @pl.when(i == SIDE_Y)
            def _():
                over_y(mat, i, top, SHORT).start()

            @pl.when(i == SIDE_Z)
            def _():
                over_z(mat, i, low, SHORT).start()
            return 0
        lax.fori_loop(0, 4, body, 0)

    def add(mat, i, base, buf, k):
        def body(t, _):
            rows = pl.ds(pl.multiple_of(t * STRIP, STRIP), STRIP)
            here = pl.ds(pl.multiple_of(base + t * STRIP, STRIP), STRIP)
            part[mat, i, here, :] = part[mat, i, here, :] + buf[mat, k, rows, :]
            return 0
        lax.fori_loop(0, HALF // STRIP, body, 0)

    for mat in range(2):
        over_y(mat, DIAG, top, LONG).wait_recv()
        add(mat, SIDE_Z, 0, ry, LONG)
        over_z(mat, SIDE_Z, top, SUMS).start()
        over_z(mat, DIAG, low, LONG).wait_recv()
        add(mat, SIDE_Y, HALF, rz, LONG)
        over_y(mat, SIDE_Y, low, SUMS).start()
    for mat in range(2):
        over_y(mat, SIDE_Y, top, SHORT).wait_recv()
        add(mat, SELF, 0, ry, SHORT)
        over_z(mat, SIDE_Z, low, SHORT).wait_recv()
        add(mat, SELF, HALF, rz, SHORT)
    outs = [pltpu.make_async_copy(part.at[mat, SELF], ref.at[0], o_sem.at[mat]) for mat, ref in ((0, r2_ref), (1, r1_ref))]
    for mat in range(2):
        over_z(mat, SIDE_Z, top, SUMS).wait_recv()
        add(mat, SELF, 0, rz, SUMS)
        over_y(mat, SIDE_Y, low, SUMS).wait_recv()
        add(mat, SELF, HALF, ry, SUMS)
        outs[mat].start()
    for mat in range(2):
        for k in (LONG, SHORT, SUMS):
            over_y(mat, DIAG, top, k).wait_send()
            over_z(mat, DIAG, top, k).wait_send()
        outs[mat].wait()


def run_reduce(act_h, grad, acts, d_pre, acc_second, acc_first):
    shard = jax.ShapeDtypeStruct((1, DIM, DIM), F32)
    return pl.pallas_call(
        reduce_kernel, in_specs=[ANY] * 6, out_specs=[ANY] * 2, out_shape=[shard, shard], name='reduce',
        scratch_shapes=[pltpu.VMEM((ROWS, DIM), BF16), pltpu.VMEM((ROWS, DIM), BF16), pltpu.VMEM((2, ROWS, DIM), BF16),
                        pltpu.VMEM((2, 4, DIM, DIM), F32), pltpu.VMEM((2, 3, HALF, DIM), F32), pltpu.VMEM((2, 3, HALF, DIM), F32),
                        DMA((2,)), DMA((2, 4)), DMA((2, 4))] + [DMA((2, 3))] * 4 + [DMA((2,))],
        cost_estimate=pl.CostEstimate(flops=150_000_000_000, bytes_accessed=70 * MIB, transcendentals=0),
        compiler_params=pltpu.CompilerParams(vmem_limit_bytes=VMEM_BIG, has_side_effects=True),
    )(act_h, grad, acts, d_pre, acc_second, acc_first)


def gelu_grad(z):
    z_sq = z * z
    t = jnp.tanh(z * (ROOT + ROOT * CUBE * z_sq))
    return 0.5 + 0.5 * t + (0.5 * z) * (1.0 - t * t) * (ROOT + 3.0 * ROOT * CUBE * z_sq)


N_CHUNK = 8


def backward_kernel(a_ref, d_ref, w1_ref, w2_ref, h_ref, dz_ref, g_ref, a_v, w1_v, w2_v, c_v, z_v, g_v, h_b, p_b, s_b,
                    in_sem, w_sem, h_sem, p_sem, o_sem, send_sem, recv_sem):
    stage = lax.axis_index('stage')
    rep = lax.axis_index('data')
    rows = a_v.shape[0] // N_CHUNK
    below = jnp.maximum(stage - 1, 0)
    cp_a = pltpu.make_async_copy(a_ref.at[0], a_v, in_sem.at[0])
    cp_a.start()

    def w_copy(i):
        span = pl.ds((i % 4) * DIM, DIM)
        src = w1_ref.at[0, :, span] if i < 4 else w2_ref.at[0, span, :]
        return pltpu.make_async_copy(src, c_v.at[i % 3], w_sem.at[i])

    for i in range(3):
        w_copy(i).start()
    n_pre = jnp.where(stage == 3, 0, jnp.where(stage == 2, 4, N_CHUNK))

    def d_copy(k):
        return pltpu.make_async_copy(d_ref.at[pl.ds(pl.multiple_of(k * rows, rows), rows)], g_v.at[k], recv_sem.at[k])

    @pl.when(stage == 3)
    def _():
        def body(k, _):
            d_copy(k).start()
            return 0
        lax.fori_loop(0, N_CHUNK, body, 0)

    def out_copy(buf, ref, sem, k):
        return pltpu.make_async_copy(buf, ref.at[pl.ds(pl.multiple_of(k * rows, rows), rows)], sem.at[k])

    def h_copy(k):
        return out_copy(h_b.at[lax.rem(k, 2)], h_ref, h_sem, k)

    def p_copy(k):
        return out_copy(p_b.at[lax.rem(k, 2)], dz_ref, p_sem, k)

    def g_copy(k):
        return out_copy(g_v.at[k], g_ref, o_sem, k)

    def send(k):
        return push(s_b.at[k], g_v.at[k], send_sem.at[k], recv_sem.at[k], rep, below)

    def z_body(k, _):
        @pl.when(k >= 2)
        def _():
            h_copy(k - 2).wait()
        a = a_v[pl.ds(pl.multiple_of(k * rows, rows), rows), :]
        slot = lax.rem(k, 2)
        for j in range(4):
            cols = slice(j * DIM, (j + 1) * DIM)
            z = jnp.dot(a, w1_v[:, cols], preferred_element_type=F32)
            z_v[k, :, cols] = z
            h_b[slot, :, cols] = gelu_kernel(z).astype(BF16)
        h_copy(k).start()
        return 0

    for i in range(8):
        w_copy(i).wait()
        span = slice((i % 4) * DIM, (i % 4 + 1) * DIM)
        if i < 4:
            w1_v[:, span] = c_v[i % 3].astype(BF16)
        else:
            w2_v[span, :] = c_v[i % 3].astype(BF16)
        if i < 5:
            w_copy(i + 3).start()
    cp_a.wait()
    lax.fori_loop(0, n_pre, z_body, 0)

    def chain_body(k, _):
        lax.fori_loop(k, jnp.where(k >= n_pre, k + 1, k), z_body, 0)
        d_copy(k).wait()

        @pl.when(k >= 2)
        def _():
            p_copy(k - 2).wait()
        g_copy(k).start()
        g = g_v[k]
        slot = lax.rem(k, 2)
        acc = None
        for j in range(4):
            cols = slice(j * DIM, (j + 1) * DIM)
            d_hid = lax.dot_general(g, w2_v[cols, :], TRANS_DIMS, preferred_element_type=F32)
            d_pre = (gelu_grad(z_v[k, :, cols]) * d_hid).astype(BF16)
            p_b[slot, :, cols] = d_pre
            part = lax.dot_general(d_pre, w1_v[:, cols], TRANS_DIMS, preferred_element_type=F32)
            acc = part if acc is None else acc + part
        s_b[k] = (g.astype(F32) + acc).astype(BF16)

        @pl.when(stage > 0)
        def _():
            send(k).start()
        p_copy(k).start()
        return 0

    lax.fori_loop(0, N_CHUNK, chain_body, 0)

    @pl.when(stage > 0)
    def _():
        def body(k, _):
            send(k).wait_send()
            return 0
        lax.fori_loop(0, N_CHUNK, body, 0)
    for k in (N_CHUNK - 2, N_CHUNK - 1):
        h_copy(k).wait()
        p_copy(k).wait()

    def fin(k, _):
        g_copy(k).wait()
        return 0
    lax.fori_loop(0, N_CHUNK, fin, 0)


def run_backward(acts, d_out, w1, w2):
    n = d_out.shape[0]
    rows = n // N_CHUNK
    return pl.pallas_call(
        backward_kernel, in_specs=[ANY] * 4, out_specs=[ANY] * 3, name='backward',
        out_shape=[jax.ShapeDtypeStruct((n, FFN), BF16), jax.ShapeDtypeStruct((n, FFN), BF16), jax.ShapeDtypeStruct((n, DIM), BF16)],
        scratch_shapes=[
            pltpu.VMEM((n, DIM), BF16), pltpu.VMEM((DIM, FFN), BF16), pltpu.VMEM((FFN, DIM), BF16), pltpu.VMEM((3, DIM, DIM), F32),
            pltpu.VMEM((N_CHUNK, rows, FFN), F32), pltpu.VMEM((N_CHUNK, rows, DIM), BF16),
            pltpu.VMEM((2, rows, FFN), BF16), pltpu.VMEM((2, rows, FFN), BF16), pltpu.VMEM((N_CHUNK, rows, DIM), BF16),
            DMA((1,)), DMA((8,)), DMA((N_CHUNK,)), DMA((N_CHUNK,)),
            DMA((N_CHUNK,)), DMA((N_CHUNK,)), DMA((N_CHUNK,))],
        cost_estimate=pl.CostEstimate(flops=6 * n * DIM * FFN, bytes_accessed=50_000_000, transcendentals=2 * n * FFN),
        compiler_params=pltpu.CompilerParams(vmem_limit_bytes=VMEM_BIG, has_side_effects=True),
    )(acts, d_out, w1, w2)


def middle_kernel(lr_ref, mx_ref, r1_ref, r2_ref, w1_ref, m1_ref, v1_ref, w2_ref, m2_ref, v2_ref, x_ref,
                  y0_ref, y1_ref, all_ref, scal_ref, r_v, p_v, q_v, s_v, n_v, w_v, x_buf, h_buf,
                  r_sem, p_sem, x_sem, ns, nr, hs, hr, xs, xr, o_sem, y_sem, *sems):
    stage, core, rep, mate, _ = ids()
    side = lax.div(stage, 2)
    base = 2 * side
    far = lax.rem(stage + 2, 4)
    me = rep * 4 + stage
    n_dev = 16
    n_tile = x_buf.shape[0] // TILE

    r_loads = [pltpu.make_async_copy(ref.at[0], r_v.at[k], r_sem.at[k]) for k, ref in enumerate((r1_ref, r2_ref))]

    def loads(turn, k):
        half = (1 - core) if turn == 0 else core
        start = pl.multiple_of(rep * DIM, DIM)
        if k == 0:
            refs, where = (w1_ref, m1_ref, v1_ref), (0, pl.ds(pl.multiple_of(half * HALF, HALF), HALF), pl.ds(start, DIM))
        else:
            refs, where = (w2_ref, m2_ref, v2_ref), (0, pl.ds(pl.multiple_of(start + half * HALF, HALF), HALF))
        return [pltpu.make_async_copy(ref.at[where], p_v.at[k, i], p_sem.at[turn, k, i]) for i, ref in enumerate(refs)]

    x_loads = [pltpu.make_async_copy(x_ref.at[4 * q + stage], x_buf.at[pl.ds(q * ROWS, ROWS)], x_sem.at[q]) for q in range(2)]
    for cp in r_loads + loads(0, 0) + loads(0, 1) + x_loads:
        cp.start()
    for cp in r_loads:
        cp.wait()

    def sq_body(t, acc):
        rows = pl.ds(pl.multiple_of(t * STRIP, STRIP), STRIP)
        a = r_v[0, rows, :]
        b = r_v[1, rows, :]
        return acc + a * a + b * b
    acc = lax.fori_loop(0, DIM // STRIP, sq_body, jnp.zeros((STRIP, DIM), F32))
    n_v[me] = jnp.full(n_v.shape[1:], jnp.sum(acc), F32)

    def norm_send(i):
        peer = lax.rem(me + i, n_dev)
        return push(n_v.at[me], n_v.at[me], ns.at[i], nr.at[i], lax.div(peer, 4), lax.rem(peer, 4))

    for i in range(1, n_dev):
        norm_send(i).start()
    for i in range(1, n_dev):
        norm_send(i).wait()
    total = n_v[0]
    for i in range(1, n_dev):
        total = total + n_v[i]
    norm = jnp.sqrt(total[:1, :1] * 0.0625)
    clip = jnp.minimum(1.0, mx_ref[0] / (norm + NORM_EPS)) * 0.25
    scal_ref[...] = jnp.broadcast_to(clip, scal_ref.shape)
    lr = lr_ref[0]

    def upd(turn, dst):
        half = (1 - core) if turn == 0 else core
        for k in range(2):
            for cp in loads(turn, k):
                cp.wait()

            def body(t, _):
                here = pl.ds(pl.multiple_of(t * STRIP, STRIP), STRIP)
                rows = pl.ds(pl.multiple_of(half * HALF + t * STRIP, STRIP), STRIP)
                new = adamw_update(p_v[k, 0, here, :], p_v[k, 1, here, :], p_v[k, 2, here, :], r_v[k, rows, :], clip, lr)[0]
                dst[k, here, :] = new.astype(BF16)
                return 0
            lax.fori_loop(0, HALF // STRIP, body, 0)
            if turn == 0:
                for cp in loads(1, k):
                    cp.start()

    upd(0, s_v)
    half_cp = push(s_v, q_v.at[stage], hs, hr, rep, mate)
    half_cp.start()
    upd(1, q_v.at[stage])
    half_cp.wait_send()
    push(s_v, q_v.at[mate], hs, hr, rep, mate).wait_recv()

    def x_part(blk, i):
        src = q_v.at[blk + i // 2, i % 2]
        return push(src, src, xs.at[i], xr.at[i], rep, far)

    x_out = [x_part(base, i) for i in range(4)]
    x_in = [x_part(2 - base, i) for i in range(4)]
    for cp in x_out:
        cp.start()

    def before(part):
        @pl.when(side == 1)
        def _():
            x_in[part].wait_recv()

    def steps_of(blk, hook=None):
        slot = lax.rem(blk, 3)
        return exchange_steps(lambda part: q_v.at[blk, part], w_v.at[slot], [sem.at[blk] for sem in sems], hook)

    for step in steps_of(0, before):
        step()

    @pl.when(side == 0)
    def _():
        x_in[0].wait_recv()
        x_in[1].wait_recv()
    x_in[2].wait_recv()
    x_in[3].wait_recv()
    for cp in x_out:
        cp.wait_send()
    for cp in x_loads:
        cp.wait()

    def keep(blk):
        return pltpu.make_async_copy(w_v.at[lax.rem(blk, 3)], all_ref.at[blk], o_sem.at[blk])

    def y_copy(t):
        rows = pl.ds(pl.multiple_of(t * TILE, TILE), TILE)
        return pltpu.make_async_copy(x_buf.at[rows], y0_ref.at[rows], y_sem.at[t])

    y1_copy = pltpu.make_async_copy(x_buf.at[pl.ds(ROWS, ROWS)], y1_ref, y_sem.at[n_tile - 1])

    def blk_body(blk, _):
        keep(blk).start()
        steps = steps_of(blk + 1)
        more = blk < 3

        def tile_body(t, _):
            for when, step in zip((0, 3, 5, 7), steps):
                pl.when(jnp.logical_and(more, t == when))(step)
            mlp_tile(x_buf, pl.ds(pl.multiple_of(t * TILE, TILE), TILE), w_v.at[lax.rem(blk, 3)], h_buf)

            @pl.when(jnp.logical_and(blk == 3, t > 0))
            def _():
                y_copy(t - 1).start()
            return 0
        lax.fori_loop(0, jnp.where(more, n_tile, n_tile // 2), tile_body, 0)

        @pl.when(more)
        def _():
            for step in steps[4:]:
                step()

        @pl.when(blk == 2)
        def _():
            y1_copy.start()
        keep(blk).wait()
        return 0

    lax.fori_loop(0, 4, blk_body, 0)
    y_copy(n_tile // 2 - 1).start()
    y1_copy.wait()
    for t in range(n_tile // 2):
        y_copy(t).wait()


def run_middle(lr, mx, r1, r2, w1, m1, v1, w2, m2, v2, x):
    smem = pl.BlockSpec(memory_space=pltpu.SMEM)
    n_rows = 2 * ROWS
    return pl.pallas_call(
        middle_kernel, in_specs=[smem, smem] + [ANY] * 9,
        out_specs=[ANY] * 3 + [pl.BlockSpec(memory_space=pltpu.VMEM)],
        out_shape=[jax.ShapeDtypeStruct((ROWS, DIM), BF16)] * 2 + [jax.ShapeDtypeStruct((4, 4, 2, DIM, DIM), BF16), jax.ShapeDtypeStruct((8, 128), F32)], name='middle',
        scratch_shapes=[
            pltpu.VMEM((2, DIM, DIM), F32), pltpu.VMEM((2, 3, HALF, DIM), F32), pltpu.VMEM((4, 2, HALF, DIM), BF16),
            pltpu.VMEM((2, HALF, DIM), BF16), pltpu.VMEM((16, 8, 128), F32), pltpu.VMEM((3, 4, 2, DIM, DIM), BF16),
            pltpu.VMEM((n_rows, DIM), BF16), pltpu.VMEM((TILE, FFN), BF16),
            DMA((2,)), DMA((2, 2, 3)), DMA((2,)), DMA((16,)), DMA((16,)), DMA, DMA, DMA((4,)), DMA((4,)), DMA((4,)), DMA((n_rows // TILE,))] + EXCHANGE_SEMS,
        cost_estimate=pl.CostEstimate(flops=200_000_000_000, bytes_accessed=100 * MIB, transcendentals=0),
        compiler_params=pltpu.CompilerParams(vmem_limit_bytes=VMEM_BIG, has_side_effects=True),
    )(lr, mx, r1, r2, w1, m1, v1, w2, m2, v2, x)


def solution(mesh):
    w_spec = P('stage', None, None)
    acc_spec = P('data', 'stage', None, None)
    row_spec = P(None, 'data', None)

    def stage_program(w_in, w_out, mom_in, mom_out, var_in, var_out, acc_in, acc_out, stage_acts, d_out, next_x, learn_rate, max_norm):
        act_h, pre_keep, grad_keep = run_backward(stage_acts, d_out, w_in, w_out)
        sh_second, sh_first = run_reduce(act_h, grad_keep, stage_acts, pre_keep, acc_out, acc_in)
        def to_mate(rows):
            return lax.ppermute(rows, 'stage', CORE_PERM)

        def to_far(rows):
            return lax.ppermute(rows, 'stage', X_PERM)

        y_0, rows_a, weights, scal = run_middle(learn_rate, max_norm, sh_first, sh_second, w_in, mom_in, var_in, w_out, mom_out, var_out, next_x)
        scal = jnp.stack([scal[0, 0], learn_rate[0]])
        sh_second, sh_first, rows_a = lax.optimization_barrier((sh_second, sh_first, rows_a))
        far_0, mate_0 = to_far(y_0), to_mate(y_0)
        y_1 = run_forward(rows_a, weights, CHUNK_0, 'fwd_a3', blocks=(3,))
        far_1, mate_1 = to_far(y_1), to_mate(y_1)
        sides = [(y_0, OWN, CHUNK_0), (y_1, OWN, CHUNK_1), (mate_0, MATE, CHUNK_0)]
        out, y_2 = run_forward(next_x, weights, CHUNK_2, 'fwd_b', to_out=True, sides=sides)
        far_0, mate_1, y_2 = lax.optimization_barrier((far_0, mate_1, y_2))
        relay_0 = to_mate(far_0)
        far_2, mate_2 = to_far(y_2), to_mate(y_2)
        sides = [(mate_1, MATE, CHUNK_1), (far_0, FAR, CHUNK_0)]
        out, y_3 = run_forward(next_x, weights, CHUNK_3, 'fwd_c', to_out=True, out_buf=out, sides=sides)
        far_1, y_3 = lax.optimization_barrier((far_1, y_3))
        relay_1 = to_mate(far_1)
        far_3, mate_3 = to_far(y_3), to_mate(y_3)
        sides = [(far_1, FAR, CHUNK_1), (relay_0, RELAY, CHUNK_0), (mate_2, MATE, CHUNK_2)]
        out, y_4 = run_forward(next_x, weights, CHUNK_4, 'fwd_d', to_out=True, out_buf=out, sides=sides)
        full_second = lax.all_gather(sh_second[0], 'data')
        full_first = lax.all_gather(sh_first[0], 'data')
        scal, y_4 = lax.optimization_barrier((scal, y_4))
        far_4, mate_4 = to_far(y_4), to_mate(y_4)
        new_second, mom_second, sec_second = run_update(scal, full_second, w_out, mom_out, var_out, 'upd_second')
        far_2, new_second, scal = lax.optimization_barrier((far_2, new_second, scal))
        relay_2 = to_mate(far_2)
        new_first, mom_first, sec_first = run_update(scal, full_first, w_in, mom_in, var_in, 'upd_first')
        far_3, new_first = lax.optimization_barrier((far_3, new_first))
        relay_3, relay_4 = to_mate(far_3), to_mate(far_4)
        out = run_copy(out, [(relay_1, RELAY, CHUNK_1), (mate_3, MATE, CHUNK_3), (far_2, FAR, CHUNK_2)], 'put_a')
        out = run_copy(out, [(relay_2, RELAY, CHUNK_2), (far_3, FAR, CHUNK_3), (relay_3, RELAY, CHUNK_3), (mate_4, MATE, CHUNK_4), (far_4, FAR, CHUNK_4), (relay_4, RELAY, CHUNK_4)], 'put_b')
        return (new_first, new_second, mom_first, mom_second, sec_first, sec_second, out)

    return jax.shard_map(stage_program, mesh=mesh, in_specs=(w_spec, w_spec, w_spec, w_spec, w_spec, w_spec, acc_spec, acc_spec, P('stage', 'data', None), P('data', None), row_spec, P(None), P(None)), out_specs=(w_spec, w_spec, w_spec, w_spec, w_spec, w_spec, row_spec), check_vma=False)
```
